32 devices in a mesh: replica: 2 (over x), model2: 4 (over z), model: 4 (over y, core).
Axes of the slice: x: 2, y: 2, z: 4, core: 2. Of those that a mesh axis runs over, the one named last changes fastest.
Arguments:
- x_prompt: bfloat16 [4, 3, 384, 2048], P('replica'), parts along dimension 0
- lengths: int32 [4, 3], P('replica'), parts along dimension 0
- x_new: bfloat16 [12, 2048], P('replica'), parts along dimension 0
- st_qkv: bfloat16 [4, 2048, 2560], P('model')
- st_out: bfloat16 [4, 2048, 2048], P('model')
- st_gateup: bfloat16 [4, 2048, 11264], P('model')
- st_down_t: bfloat16 [4, 2048, 5632], P('model')
- gain_attn: float32 [4, 2048], replicated
- gain_mlp: float32 [4, 2048], replicated
- tp_query: bfloat16 [4, 2048, 32, 64], P(None, None, ('model', 'model2'))
- tp_key: bfloat16 [4, 2048, 16, 64], P(None, None, ('model', 'model2'))
- tp_value: bfloat16 [4, 2048, 16, 64], P(None, None, ('model', 'model2'))
- tp_out: bfloat16 [4, 32, 64, 2048], P(None, ('model', 'model2'))
- tp_gate: bfloat16 [4, 2048, 5632], P(None, None, ('model', 'model2'))
- tp_up: bfloat16 [4, 2048, 5632], P(None, None, ('model', 'model2'))
- tp_down: bfloat16 [4, 5632, 2048], P(None, ('model', 'model2'))
Outputs:
- output 1: bfloat16 [12, 2048], P('replica'), parts along dimension 0
- output 2: bfloat16 [12, 2048], P('replica'), parts along dimension 0
- output 3: bfloat16 [4, 12, 385, 16, 64], P(None, 'replica', None, ('model', 'model2')), parts along dimension 1
- output 4: bfloat16 [4, 12, 385, 16, 64], P(None, 'replica', None, ('model', 'model2')), parts along dimension 1
There are 2 independent parts. The reference program is written for one: setup_inputs(seed, part) draws one part's arguments, and reference() takes and returns one part's arrays. A program takes and returns all parts, laid end to end along the dimension named above; an argument that names none is the same for every part.
All inputs are finite; a program needn't handle non-finite values.
Results may differ from the reference program's by a relative error of at most 0.0165032.
Values are sent between devices in bfloat16 or wider.
A program may use at most 1 GiB of HBM per device.

```python
import jax
import jax.numpy as jnp
from jax import lax

D = 2048
HEADS = 32
KV_HEADS = 4
HEAD = 64
FF = 5632
LAYERS = 4
MICROBATCHES = 2
MICRO_ROWS = 3
BATCH = 6
SEQ_LEN = 384
SLOTS = 16
EPS = 1e-5
THETA = 10000.0


def rms_norm(values_in, gain_vec):
    x_f32 = values_in.astype(jnp.float32)
    inv_rms = lax.rsqrt(jnp.mean(x_f32 * x_f32, axis=-1, keepdims=True) + EPS)
    return (x_f32 * inv_rms * gain_vec).astype(jnp.bfloat16)


def rope_angles(positions):
    half_dim = HEAD // 2
    inv_freq = jnp.power(THETA, jnp.arange(half_dim, dtype=jnp.float32) * (-2.0 / HEAD))
    angles = positions.astype(jnp.float32)[..., None] * inv_freq
    return jnp.cos(angles), jnp.sin(angles)


def apply_rope(values_in, cos_t, sin_t):
    half_dim = values_in.shape[-1] // 2
    first_half = values_in[..., :half_dim]
    second = values_in[..., half_dim:]
    return jnp.concatenate([first_half * cos_t - second * sin_t, second * cos_t + first_half * sin_t], axis=-1)


def draw_lengths(len_key):
    drawn = jax.random.randint(len_key, (BATCH,), SEQ_LEN // 4, SEQ_LEN + 1)
    if BATCH > 1:
        drawn = drawn.at[BATCH - 1].set(SEQ_LEN)
    return drawn.reshape(MICROBATCHES, MICRO_ROWS).astype(jnp.int32)


def setup_inputs(seed: int = 0, part: int = 0) -> dict:
    base_key = jax.random.key(seed)
    shared = jax.random.split(base_key, 7)
    own = jax.random.split(jax.random.fold_in(base_key, part), 4)
    q_cols = HEADS * HEAD
    k_cols = KV_HEADS * HEAD
    w_qkv = (jax.random.normal(shared[0], (LAYERS, D, q_cols + 2 * k_cols), jnp.float32) * D ** -0.5).astype(jnp.bfloat16)
    w_out = (jax.random.normal(shared[1], (LAYERS, q_cols, D), jnp.float32) * q_cols ** -0.5).astype(jnp.bfloat16)
    w_gate = (jax.random.normal(shared[2], (LAYERS, D, FF), jnp.float32) * D ** -0.5).astype(jnp.bfloat16)
    w_up = (jax.random.normal(shared[3], (LAYERS, D, FF), jnp.float32) * D ** -0.5).astype(jnp.bfloat16)
    w_down = (jax.random.normal(shared[4], (LAYERS, FF, D), jnp.float32) * FF ** -0.5).astype(jnp.bfloat16)
    gain_attn = jax.random.uniform(shared[5], (LAYERS, D), jnp.float32, 0.5, 1.5)
    gain_mlp = jax.random.uniform(shared[6], (LAYERS, D), jnp.float32, 0.5, 1.5)
    row_mean = jax.random.normal(own[0], (BATCH, 1, D), jnp.float32)
    x_prompt = (jax.random.normal(own[1], (BATCH, SEQ_LEN, D), jnp.float32) + row_mean).astype(jnp.bfloat16).reshape(MICROBATCHES, MICRO_ROWS, SEQ_LEN, D)
    x_new = jax.random.normal(own[2], (BATCH, D), jnp.float32).astype(jnp.bfloat16)
    lengths = draw_lengths(own[3])
    rep_factor = SLOTS // KV_HEADS
    k_part = w_qkv[:, :, q_cols:q_cols + k_cols].reshape(LAYERS, D, KV_HEADS, HEAD)
    v_part = w_qkv[:, :, q_cols + k_cols:].reshape(LAYERS, D, KV_HEADS, HEAD)
    return {
        'x_prompt': x_prompt,
        'lengths': lengths,
        'x_new': x_new,
        'st_qkv': w_qkv,
        'st_out': w_out,
        'st_gateup': jnp.concatenate([w_gate, w_up], axis=2),
        'st_down_t': jnp.swapaxes(w_down, 1, 2),
        'gain_attn': gain_attn,
        'gain_mlp': gain_mlp,
        'tp_query': w_qkv[:, :, :q_cols].reshape(LAYERS, D, HEADS, HEAD),
        'tp_key': jnp.repeat(k_part, rep_factor, axis=2),
        'tp_value': jnp.repeat(v_part, rep_factor, axis=2),
        'tp_out': w_out.reshape(LAYERS, HEADS, HEAD, D),
        'tp_gate': w_gate,
        'tp_up': w_up,
        'tp_down': w_down,
    }


def prefill_row(x_row, length, st_qkv, st_out, st_gateup, st_down_t, gain_attn, gain_mlp):
    q_cols = HEADS * HEAD
    k_cols = KV_HEADS * HEAD
    group_size = HEADS // KV_HEADS
    positions = jnp.arange(SEQ_LEN)
    cos_t, sin_t = rope_angles(positions)
    key_mask = (positions[None, :] <= positions[:, None]) & (positions[None, :] < length)

    def layer_fn(hidden_x, params):
        g_attn, g_mlp, w_qkv, w_out, w_gateup, w_down_t = params
        normed = rms_norm(hidden_x, g_attn)
        proj_all = jnp.dot(normed, w_qkv, preferred_element_type=jnp.float32)
        queries = apply_rope(proj_all[:, :q_cols].reshape(SEQ_LEN, KV_HEADS, group_size, HEAD), cos_t[:, None, None, :], sin_t[:, None, None, :]).astype(jnp.bfloat16)
        key_rot = apply_rope(proj_all[:, q_cols:q_cols + k_cols].reshape(SEQ_LEN, KV_HEADS, HEAD), cos_t[:, None, :], sin_t[:, None, :]).astype(jnp.bfloat16)
        val_proj = proj_all[:, q_cols + k_cols:].reshape(SEQ_LEN, KV_HEADS, HEAD).astype(jnp.bfloat16)
        scores = jnp.einsum('qcge,kce->cgqk', queries.astype(jnp.float32), key_rot.astype(jnp.float32)) * HEAD ** -0.5
        scores = jnp.where(key_mask, scores, -1e30)
        probs_bf = jax.nn.softmax(scores, axis=-1).astype(jnp.bfloat16)
        attn_out = jnp.einsum('cgqk,kce->qcge', probs_bf.astype(jnp.float32), val_proj.astype(jnp.float32)).astype(jnp.bfloat16).reshape(SEQ_LEN, q_cols)
        resid_mid = (hidden_x.astype(jnp.float32) + jnp.dot(attn_out, w_out, preferred_element_type=jnp.float32)).astype(jnp.bfloat16)
        normed_mlp = rms_norm(resid_mid, g_mlp)
        gate_up = jnp.dot(normed_mlp, w_gateup, preferred_element_type=jnp.float32)
        act_out = (jax.nn.silu(gate_up[:, :FF]) * gate_up[:, FF:]).astype(jnp.bfloat16)
        layer_out = (resid_mid.astype(jnp.float32) + jnp.dot(act_out, w_down_t.T, preferred_element_type=jnp.float32)).astype(jnp.bfloat16)
        return layer_out, (key_rot, val_proj)

    final_x, kv_pair = lax.scan(layer_fn, x_row, (gain_attn, gain_mlp, st_qkv, st_out, st_gateup, st_down_t))
    last_row = lax.dynamic_index_in_dim(final_x, length - 1, axis=0, keepdims=False)
    return last_row, kv_pair[0], kv_pair[1]


def reference(x_prompt, lengths, x_new, st_qkv, st_out, st_gateup, st_down_t, gain_attn, gain_mlp, tp_query, tp_key, tp_value, tp_out, tp_gate, tp_up, tp_down):
    rows_x = x_prompt.reshape(BATCH, SEQ_LEN, D)
    len_flat = lengths.reshape(BATCH)
    last_hidden, k_rows, v_rows = lax.map(lambda row_pair: prefill_row(row_pair[0], row_pair[1], st_qkv, st_out, st_gateup, st_down_t, gain_attn, gain_mlp), (rows_x, len_flat))
    rep_factor = SLOTS // KV_HEADS
    k_cache = jnp.repeat(jnp.swapaxes(k_rows, 0, 1), rep_factor, axis=3)
    v_cache = jnp.repeat(jnp.swapaxes(v_rows, 0, 1), rep_factor, axis=3)
    group_slot = HEADS // SLOTS
    cos_n, sin_n = rope_angles(len_flat)
    cached = jnp.arange(SEQ_LEN)[None, :] < len_flat[:, None]
    score_scale = HEAD ** -0.5

    def dec_layer(hidden_x, params):
        g_attn, g_mlp, w_query, w_key, w_value, w_outp, w_gate, w_upp, w_down, k_cached, v_cached = params
        normed = rms_norm(hidden_x, g_attn)
        normed_f = normed.astype(jnp.float32)
        queries = apply_rope(jnp.einsum('bd,dhe->bhe', normed_f, w_query.astype(jnp.float32)), cos_n[:, None, :], sin_n[:, None, :])
        queries = queries.astype(jnp.bfloat16).reshape(BATCH, SLOTS, group_slot, HEAD).astype(jnp.float32)
        key_new = apply_rope(jnp.einsum('bd,dce->bce', normed_f, w_key.astype(jnp.float32)), cos_n[:, None, :], sin_n[:, None, :]).astype(jnp.bfloat16)
        val_new = jnp.einsum('bd,dce->bce', normed_f, w_value.astype(jnp.float32)).astype(jnp.bfloat16)
        s_old = jnp.einsum('bcge,bsce->bcgs', queries, k_cached.astype(jnp.float32)) * score_scale
        s_old = jnp.where(cached[:, None, None, :], s_old, -1e30)
        s_new = jnp.einsum('bcge,bce->bcg', queries, key_new.astype(jnp.float32)) * score_scale
        row_max = jnp.maximum(jnp.max(s_old, axis=-1), s_new)
        e_old = jnp.exp(s_old - row_max[..., None])
        e_new = jnp.exp(s_new - row_max)
        denom_sum = jnp.sum(e_old, axis=-1) + e_new
        p_old = (e_old / denom_sum[..., None]).astype(jnp.bfloat16)
        p_new = (e_new / denom_sum).astype(jnp.bfloat16)
        attn_out = jnp.einsum('bcgs,bsce->bcge', p_old.astype(jnp.float32), v_cached.astype(jnp.float32)) + p_new.astype(jnp.float32)[..., None] * val_new.astype(jnp.float32)[:, :, None, :]
        attn_out = attn_out.astype(jnp.bfloat16).reshape(BATCH, HEADS, HEAD)
        resid_mid = (hidden_x.astype(jnp.float32) + jnp.einsum('bhe,hed->bd', attn_out.astype(jnp.float32), w_outp.astype(jnp.float32))).astype(jnp.bfloat16)
        normed_mlp = rms_norm(resid_mid, g_mlp)
        act_out = (jax.nn.silu(jnp.dot(normed_mlp, w_gate, preferred_element_type=jnp.float32)) * jnp.dot(normed_mlp, w_upp, preferred_element_type=jnp.float32)).astype(jnp.bfloat16)
        layer_out = (resid_mid.astype(jnp.float32) + jnp.dot(act_out, w_down, preferred_element_type=jnp.float32)).astype(jnp.bfloat16)
        return layer_out, (key_new, val_new)

    dec_out, new_kv = lax.scan(dec_layer, x_new, (gain_attn, gain_mlp, tp_query, tp_key, tp_value, tp_out, tp_gate, tp_up, tp_down, k_cache, v_cache))
    k_full = jnp.concatenate([k_cache, new_kv[0][:, :, None]], axis=2)
    v_full = jnp.concatenate([v_cache, new_kv[1][:, :, None]], axis=2)
    return (dec_out, last_hidden, k_full, v_full)
```

```python
import jax
import jax.numpy as jnp
import numpy as np
from jax import lax
from jax.sharding import PartitionSpec as P

EPS = 1e-5
THETA = 10000.0
TP_AXES = ('model', 'model2')
NEG = -1e30

CHUNKS = (((4, 0), (1, 0), (5, 0), (3, 0)),
          ((0, 0), (1, 1), (2, 0), (3, 1)),
          ((0, 1), (4, 1), (2, 1), (5, 1)))


def rms_norm(values_in, gain_vec):
    x_f32 = values_in.astype(jnp.float32)
    inv_rms = lax.rsqrt(jnp.mean(x_f32 * x_f32, axis=-1, keepdims=True) + EPS)
    return (x_f32 * inv_rms * gain_vec).astype(jnp.bfloat16)


def rope_angles(positions, head_dim):
    half_dim = head_dim // 2
    inv_freq = jnp.power(THETA, jnp.arange(half_dim, dtype=jnp.float32) * (-2.0 / head_dim))
    angles = positions.astype(jnp.float32)[..., None] * inv_freq
    return jnp.cos(angles), jnp.sin(angles)


def apply_rope(values_in, cos_t, sin_t):
    half_dim = values_in.shape[-1] // 2
    first_half = values_in[..., :half_dim]
    second = values_in[..., half_dim:]
    return jnp.concatenate([first_half * cos_t - second * sin_t, second * cos_t + first_half * sin_t], axis=-1)


def dot32(a, b):
    return jnp.dot(a, b, preferred_element_type=jnp.float32)


def rope_flat(values_in, cos_t, sin_t, head_dim):
    rows, cols = values_in.shape
    v = values_in.reshape(rows, cols // head_dim, head_dim)
    return apply_rope(v, cos_t[:, None, :], sin_t[:, None, :]).astype(jnp.bfloat16).reshape(rows, cols)


def attend(q, keys, vals, mask, head_dim):
    rows = q.shape[0]
    kv_heads = keys.shape[1] // head_dim
    group = q.shape[1] // (kv_heads * head_dim)
    qh = q.reshape(rows, kv_heads, group, head_dim)
    kh = keys.reshape(-1, kv_heads, head_dim)
    vh = vals.reshape(-1, kv_heads, head_dim)
    scores = jnp.einsum('qcge,kce->cgqk', qh, kh, preferred_element_type=jnp.float32) * head_dim ** -0.5
    scores = jnp.where(mask[None, None], scores, NEG)
    probs = jax.nn.softmax(scores, axis=-1).astype(jnp.bfloat16)
    out = jnp.einsum('cgqk,kce->qcge', probs, vh, preferred_element_type=jnp.float32)
    return out.astype(jnp.bfloat16).reshape(rows, -1)


def finish(x, o, g_mlp, w_out, w_gateup, w_down_t):
    ff = w_down_t.shape[1]
    x1 = (x.astype(jnp.float32) + dot32(o, w_out)).astype(jnp.bfloat16)
    h2 = rms_norm(x1, g_mlp)
    gu = dot32(h2, w_gateup)
    act = (jax.nn.silu(gu[:, :ff]) * gu[:, ff:]).astype(jnp.bfloat16)
    down = lax.dot_general(act, w_down_t, (((1,), (1,)), ((), ())), preferred_element_type=jnp.float32)
    return (x1.astype(jnp.float32) + down).astype(jnp.bfloat16)


def solution(mesh):
    stages = mesh.shape['model']
    width = mesh.shape['model2']
    stage_spec = P('model', None, None)
    in_specs = (P('replica', None, None, None), P('replica', None), P('replica', None),
                stage_spec, stage_spec, stage_spec, stage_spec, P(None, None), P(None, None),
                P(None, None, TP_AXES, None), P(None, None, TP_AXES, None), P(None, None, TP_AXES, None),
                P(None, TP_AXES, None, None), P(None, None, TP_AXES), P(None, None, TP_AXES), P(None, TP_AXES, None))
    cache_spec = P(None, 'replica', None, TP_AXES, None)
    out_specs = (P('replica', None), P('replica', None), cache_spec, cache_spec)
    num_k = len(CHUNKS)
    pid_tab = np.array([[c[0] for c in row] for row in CHUNKS], np.int32)
    half_tab = np.array([[c[1] for c in row] for row in CHUNKS], np.int32)

    def shard_body(x_prompt, lengths, x_new, st_qkv, st_out, st_gateup, st_down_t, gain_attn, gain_mlp, tp_query, tp_key, tp_value, tp_out, tp_gate, tp_up, tp_down):
        seq_len, model_dim = x_prompt.shape[2:]
        batch = x_new.shape[0]
        head_dim = tp_query.shape[-1]
        w_qkv, w_out, w_gateup, w_down_t = st_qkv[0], st_out[0], st_gateup[0], st_down_t[0]
        q_cols = w_out.shape[0]
        k_cols = (w_qkv.shape[1] - q_cols) // 2
        kv_heads = k_cols // head_dim
        chunk = seq_len // 2
        rows = chunk + 16
        stage = lax.axis_index('model')
        col = lax.axis_index('model2')
        g_attn = lax.dynamic_index_in_dim(gain_attn, stage, 0, keepdims=False)
        g_mlp = lax.dynamic_index_in_dim(gain_mlp, stage, 0, keepdims=False)
        lens = lengths.reshape(batch)
        x_chunks = x_prompt.reshape(batch, 2, chunk, model_dim)
        pids = jnp.asarray(pid_tab)[:, col]
        halves = jnp.asarray(half_tab)[:, col]
        row_i = jnp.arange(rows)
        key_j = jnp.arange(chunk + rows)
        send_pairs = [(i, i + 1) for i in range(stages - 1)]
        pair_z = [(i, i + 1) for i in range(0, width, 2)]

        def fresh(k):
            body = x_chunks[pids[k], halves[k]]
            new_row = x_new[pids[k]]
            return jnp.concatenate([body, new_row[None], jnp.zeros((rows - chunk - 1, model_dim), jnp.bfloat16)], axis=0)

        def tick(carry, t):
            recv, prev_kv, nb_kv, kv_store, xsel, osel = carry
            k_raw = t - stage
            valid = (k_raw >= 0) & (k_raw < num_k)
            k = jnp.clip(k_raw, 0, num_k - 1)
            x = jnp.where(stage == 0, fresh(k), recv)
            length = lens[pids[k]]
            half = halves[k]
            pos = jnp.where(row_i < chunk, half * chunk + row_i, length)
            cos_t, sin_t = rope_angles(pos, head_dim)
            ctx = jnp.where((k == num_k - 1) & (col % 2 == 1), nb_kv, prev_kv)
            is_dec = row_i >= chunk
            own = key_j - chunk
            kpos = jnp.where(key_j < chunk, key_j, half * chunk + own)
            seen_ctx = (half == 1) & (key_j < chunk)
            seen_own = (own >= 0) & (own < chunk)
            mask = (seen_ctx | seen_own)[None] & (kpos[None] < length) & (is_dec[:, None] | (kpos[None] <= pos[:, None]))
            mask = mask | (is_dec[:, None] & (own == chunk)[None])

            def full(_):
                h = rms_norm(x, g_attn)
                qkv = dot32(h, w_qkv)
                q = rope_flat(qkv[:, :q_cols], cos_t, sin_t, head_dim)
                kk = rope_flat(qkv[:, q_cols:q_cols + k_cols], cos_t, sin_t, head_dim)
                vv = qkv[:, q_cols + k_cols:].astype(jnp.bfloat16)
                kv = jnp.concatenate([kk, vv], axis=1)
                allkv = jnp.concatenate([ctx, kv], axis=0)
                o = attend(q, allkv[:, :k_cols], allkv[:, k_cols:], mask, head_dim)
                y = finish(x, o, g_mlp, w_out, w_gateup, w_down_t)
                return y, kv, jnp.zeros((16, model_dim), jnp.bfloat16), jnp.zeros((16, q_cols), jnp.bfloat16)

            def light(_):
                h = rms_norm(x, g_attn)
                kvp = dot32(h, w_qkv[:, q_cols:])
                kk = rope_flat(kvp[:, :k_cols], cos_t, sin_t, head_dim)
                kv = jnp.concatenate([kk, kvp[:, k_cols:].astype(jnp.bfloat16)], axis=1)
                allkv = jnp.concatenate([ctx, kv], axis=0)
                last_i = jnp.clip(length - 1 - half * chunk, 0, chunk - 1)
                sel = jnp.where(jnp.arange(16) == 0, last_i, chunk)
                hs = h[sel]
                q = rope_flat(dot32(hs, w_qkv[:, :q_cols]), cos_t[sel], sin_t[sel], head_dim)
                o = attend(q, allkv[:, :k_cols], allkv[:, k_cols:], mask[sel], head_dim)
                return x, kv, x[sel], o

            y, kv, xs, osx = lax.cond(stage == stages - 1, light, full, None)
            recv = lax.ppermute(y, 'model', send_pairs)
            nb_new = lax.ppermute(kv[:chunk], 'model2', pair_z)
            nb_kv = jnp.where(k_raw == 0, nb_new, nb_kv)
            upd = lambda store, new: lax.dynamic_update_index_in_dim(store, jnp.where(valid, new, lax.dynamic_index_in_dim(store, k, 0, keepdims=False)), k, 0)
            return (recv, kv[:chunk], nb_kv, upd(kv_store, kv), upd(xsel, xs), upd(osel, osx)), None

        zkv = jnp.zeros((chunk, 2 * k_cols), jnp.bfloat16)
        init = (jnp.zeros((rows, model_dim), jnp.bfloat16), zkv, zkv,
                jnp.zeros((num_k, rows, 2 * k_cols), jnp.bfloat16),
                jnp.zeros((num_k, 16, model_dim), jnp.bfloat16), jnp.zeros((num_k, 16, q_cols), jnp.bfloat16))
        final = lax.scan(tick, init, jnp.arange(num_k + stages - 1))[0]
        _, _, _, kv_store, xsel, osel = final

        x6 = xsel[:, :2].reshape(2 * num_k, model_dim)
        o6 = osel[:, :2].reshape(2 * num_k, q_cols)
        y6 = lax.cond(stage == stages - 1, lambda: finish(x6, o6, g_mlp, w_out, w_gateup, w_down_t), lambda: x6)
        rows_all = lax.all_gather(y6, TP_AXES)[(stages - 1) * width:]
        rows_all = rows_all.reshape(width, num_k, 2, model_dim)
        where_a = {}
        where_b = {}
        for k in range(num_k):
            for z in range(width):
                (where_b if CHUNKS[k][z][1] else where_a)[CHUNKS[k][z][0]] = (z, k)
        dec = jnp.stack([rows_all[where_b[p] + (1,)] for p in range(batch)])
        last = jnp.stack([jnp.where(lens[p] > chunk, rows_all[where_b[p] + (0,)], rows_all[where_a[p] + (0,)]) for p in range(batch)])

        packed = jnp.stack([jnp.concatenate([kv_store[:, :, h * head_dim:(h + 1) * head_dim],
                                             kv_store[:, :, k_cols + h * head_dim:k_cols + (h + 1) * head_dim]], axis=-1)
                            for h in range(kv_heads)])
        moved = lax.all_to_all(packed, 'model', 0, 0, tiled=True)
        spread = lax.all_gather(moved, 'model2')
        full_kv = jnp.stack([jnp.concatenate([spread[where_a[p][0], :, where_a[p][1], :chunk],
                                              spread[where_b[p][0], :, where_b[p][1], :chunk + 1]], axis=1)
                             for p in range(batch)], axis=1)
        k_full = full_kv[:, :, :, None, :head_dim]
        v_full = full_kv[:, :, :, None, head_dim:]
        return dec, last, k_full, v_full

    return jax.shard_map(shard_body, mesh=mesh, in_specs=in_specs, out_specs=out_specs, check_vma=False)
```

```python
import functools

import jax
import jax.numpy as jnp
import numpy as np
from jax import lax
from jax.experimental import pallas as pl
from jax.experimental.pallas import tpu as pltpu
from jax.sharding import PartitionSpec as P

EPS = 1e-5
THETA = 10000.0
TP_AXES = ('model', 'model2')
NEG = -1e30
BLK = 512
NBUF = 18
KEYS = 512
MESH_ID = pl.DeviceIdType.MESH

CHUNKS = (((4, 0), (1, 0), (5, 0), (3, 0)),
          ((0, 0), (1, 1), (2, 0), (3, 1)),
          ((0, 1), (4, 1), (2, 1), (5, 1)))


def rope_angles(positions, head_dim):
    half_dim = head_dim // 2
    inv_freq = jnp.power(THETA, jnp.arange(half_dim, dtype=jnp.float32) * (-2.0 / head_dim))
    angles = positions.astype(jnp.float32)[..., None] * inv_freq
    return jnp.cos(angles), jnp.sin(angles)


def dot32(a, b):
    return jnp.dot(a, b, preferred_element_type=jnp.float32)


def dot32t(a, b):
    return lax.dot_general(a, b, (((1,), (1,)), ((), ())), preferred_element_type=jnp.float32)


def norm_rows(x_f32, gain):
    inv_rms = lax.rsqrt(jnp.mean(x_f32 * x_f32, axis=-1, keepdims=True) + EPS)
    return (x_f32 * inv_rms * gain).astype(jnp.bfloat16)


def rope_block(v, cos_t, sin_t):
    lane = lax.broadcasted_iota(jnp.int32, (v.shape[0], 128), 1)
    first = (lane % 64) < 32
    out = []
    for c in range(v.shape[1] // 128):
        t = v[:, c * 128:(c + 1) * 128]
        other = jnp.where(first, pltpu.roll(t, 96, 1), pltpu.roll(t, 32, 1))
        out.append(t * cos_t + other * sin_t)
    return out


def mega_kernel(dims, x_mine, cos_ref, sin_ref, mask_ref, sel_ref, cosl_ref, sinl_ref, maskl_ref, ga_ref, gm_ref,
                w_qkv, w_out, w_gu, w_dt, kv_out, rows_out,
                wbuf, xin, ysend, kvst, nb, kst, vst, qbuf, obuf, hbuf, x1buf, yacc, hsel, x6, o6, rowbuf,
                wsem, act_send, act_recv, kv_send, kv_recv, kv_self, nb_send, nb_recv, row_send, row_recv, row_self):
    stages, width, num_k, rows, chunk, model_dim, q_cols, ff = dims
    n_dev = stages * width
    n_q = q_cols // BLK
    n_o = model_dim // BLK
    n_f = ff // BLK
    per = n_q + 1 + n_o + 3 * n_f
    stage = lax.axis_index('model')
    col = lax.axis_index('model2')
    me = stage * width + col
    last_stage = stages - 1
    f32 = jnp.float32
    bf16 = jnp.bfloat16

    def wslot(g):
        return lax.rem(g, NBUF)

    def fetch(g):
        b = lax.rem(g, per)
        slot = wslot(g)

        def go(src, j):
            pltpu.make_async_copy(src.at[:, pl.ds(pl.multiple_of(j * BLK, BLK), BLK)], wbuf.at[slot], wsem.at[slot]).start()

        @pl.when(b == 0)
        def _():
            go(w_qkv, n_q)

        @pl.when((b >= 1) & (b <= n_q))
        def _():
            go(w_qkv, b - 1)

        @pl.when((b > n_q) & (b <= n_q + n_o))
        def _():
            go(w_out, b - n_q - 1)

        f = b - (n_q + n_o + 1)

        @pl.when((f >= 0) & (lax.rem(f, 3) == 0))
        def _():
            go(w_gu, f // 3)

        @pl.when((f >= 0) & (lax.rem(f, 3) == 1))
        def _():
            go(w_gu, n_f + f // 3)

        @pl.when((f >= 0) & (lax.rem(f, 3) == 2))
        def _():
            go(w_dt, f // 3)

    def landed(g):
        slot = wslot(g)
        pltpu.make_async_copy(w_out.at[:, pl.ds(0, BLK)], wbuf.at[slot], wsem.at[slot]).wait()
        return slot

    def refill(g, total):
        @pl.when(g + NBUF < total)
        def _():
            fetch(g + NBUF)

    def first_fetch(g, carry):
        fetch(g)
        return carry
    lax.fori_loop(0, NBUF, first_fetch, 0)

    @pl.when(stage == 0)
    def _():
        for k in range(num_k):
            pltpu.make_async_copy(x_mine.at[k], xin.at[k], act_recv.at[k]).start()

    barrier = pltpu.get_barrier_semaphore()

    def peer(d):
        t = lax.rem(me + d, n_dev)
        return t // width, lax.rem(t, width)

    def greet(d, carry):
        c, z = peer(d)
        pl.semaphore_signal(barrier, inc=1, device_id={'model': c, 'model2': z}, device_id_type=MESH_ID)
        return carry
    lax.fori_loop(1, n_dev, greet, 0)

    kst[...] = jnp.zeros_like(kst)
    vst[...] = jnp.zeros_like(vst)

    def wait_x(k):
        @pl.when(stage == 0)
        def _():
            pltpu.make_async_copy(x_mine.at[k], xin.at[k], act_recv.at[k]).wait()

        @pl.when(stage > 0)
        def _():
            act_copy(k).wait_recv()

    def act_copy(k):
        return pltpu.make_async_remote_copy(src_ref=ysend.at[k], dst_ref=xin.at[k], send_sem=act_send.at[k], recv_sem=act_recv.at[k],
                                            device_id={'model': lax.rem(stage + 1, stages)}, device_id_type=MESH_ID)

    def kv_copy(k, d, src_dev):
        c, z = peer(d)
        return pltpu.make_async_remote_copy(src_ref=kvst.at[k, c], dst_ref=kv_out.at[src_dev // width, lax.rem(src_dev, width), k],
                                            send_sem=kv_send.at[k * n_dev + d], recv_sem=kv_recv.at[src_dev * num_k + k],
                                            device_id={'model': c, 'model2': z}, device_id_type=MESH_ID)

    def kv_local(k):
        return pltpu.make_async_copy(kvst.at[k, stage], kv_out.at[stage, col, k], kv_self.at[k])

    def nb_copy():
        return pltpu.make_async_remote_copy(src_ref=kvst.at[0], dst_ref=nb, send_sem=nb_send, recv_sem=nb_recv,
                                            device_id={'model2': lax.rem(col + 1, width)}, device_id_type=MESH_ID)

    def row_copy(d, src_col=None):
        c, z = peer(d)
        src = col if src_col is None else src_col
        return pltpu.make_async_remote_copy(src_ref=rowbuf, dst_ref=rows_out.at[src], send_sem=row_send.at[d], recv_sem=row_recv.at[src],
                                            device_id={'model': c, 'model2': z}, device_id_type=MESH_ID)

    lane_r = lax.broadcasted_iota(jnp.int32, (rows, 128), 1)
    low = lane_r < 64

    def stack(c, base, packed):
        n = packed.shape[0]
        lo = low[:n]
        turned = pltpu.roll(packed, 64, 1)
        zero = jnp.zeros_like(packed)
        kst[c, base:base + n, :] = jnp.where(lo, packed, zero).astype(bf16)
        kst[c, KEYS + base:KEYS + base + n, :] = jnp.where(lo, zero, turned).astype(bf16)
        vst[c, base:base + n, :] = jnp.where(lo, turned, zero).astype(bf16)
        vst[c, KEYS + base:KEYS + base + n, :] = jnp.where(lo, zero, packed).astype(bf16)

    def keys_values(k, slot):
        kv = dot32(hbuf[...], wbuf[slot])
        half = kv.shape[1] // 2
        keys = rope_block(kv[:, :half], cos_ref[k], sin_ref[k])
        for c in range(stages):
            kt = keys[c // 2]
            vt = kv[:, half + (c // 2) * 128:half + (c // 2 + 1) * 128]
            if c % 2 == 0:
                packed = jnp.where(low, kt, pltpu.roll(vt, 64, 1))
            else:
                packed = jnp.where(low, pltpu.roll(kt, 64, 1), vt)
            packed = packed.astype(bf16)
            kvst[k, c] = packed
            stack(c, chunk, packed.astype(f32))

        @pl.when(k == 0)
        def _():
            pl.semaphore_wait(barrier, n_dev - 1)

            @pl.when(lax.rem(col, 2) == 0)
            def _():
                nb_copy().start()

        def send(d, carry):
            kv_copy(k, d, me).start()
            return carry
        lax.fori_loop(1, n_dev, send, 0)
        kv_local(k).start()

        use_nb = (k == num_k - 1) & (lax.rem(col, 2) == 1)

        @pl.when(use_nb)
        def _():
            nb_copy().wait_recv()
            for c in range(stages):
                stack(c, 0, nb[c, :chunk].astype(f32))

        @pl.when((k > 0) & jnp.logical_not(use_nb))
        def _():
            for c in range(stages):
                stack(c, 0, kvst[lax.max(k - 1, 0), c, :chunk].astype(f32))

    def attend(q_ref, o_ref, m_ref, n_rows):
        pairs = q_cols // 128
        per_c = pairs // stages

        def pair(i, carry):
            c = i // per_c
            at = pl.ds(pl.multiple_of(i * 128, 128), 128)
            s = dot32t(q_ref[:, at], kst[c])
            parts = []
            for e in range(2):
                se = jnp.where(m_ref[...] > 0.5, s[:, e * KEYS:(e + 1) * KEYS], NEG)
                ex = jnp.exp(se - jnp.max(se, axis=-1, keepdims=True))
                inv = 1.0 / jnp.sum(ex, axis=-1, keepdims=True)
                parts.append((ex * inv).astype(bf16))
            o_ref[:, at] = dot32(jnp.concatenate(parts, axis=1), vst[c]).astype(bf16)
            return carry
        lax.fori_loop(0, pairs, pair, 0)

    scale = 64 ** -0.5

    def block_at(j):
        return pl.ds(pl.multiple_of(j * BLK, BLK), BLK)

    def act_of(h, slot_g, slot_u):
        g = dot32(h, wbuf[slot_g])
        u = dot32(h, wbuf[slot_u])
        return (g * jax.nn.sigmoid(g) * u).astype(bf16)

    @pl.when(stage < last_stage)
    def _():
        total = per * num_k

        def one_chunk(k, carry):
            g0 = k * per
            wait_x(k)
            hbuf[...] = norm_rows(xin[k].astype(f32), ga_ref[...])
            keys_values(k, landed(g0))
            refill(g0, total)

            def q_block(j, cc):
                g = g0 + 1 + j
                slot = landed(g)
                v = rope_block(dot32(hbuf[...], wbuf[slot]), cos_ref[k], sin_ref[k])
                for i in range(BLK // 128):
                    qbuf[:, pl.ds(pl.multiple_of(j * BLK + i * 128, 128), 128)] = (v[i] * scale).astype(bf16)
                refill(g, total)
                return cc
            lax.fori_loop(0, n_q, q_block, 0)

            attend(qbuf, obuf, mask_ref.at[k], rows)

            def o_block(j, cc):
                g = g0 + 1 + n_q + j
                slot = landed(g)
                x1buf[:, block_at(j)] = (xin[k, :, block_at(j)].astype(f32) + dot32(obuf[...], wbuf[slot])).astype(bf16)
                refill(g, total)
                return cc
            lax.fori_loop(0, n_o, o_block, 0)

            x1 = x1buf[...].astype(f32)
            hbuf[...] = norm_rows(x1, gm_ref[...])
            yacc[...] = jnp.zeros_like(yacc)

            def f_block(j, cc):
                g = g0 + 1 + n_q + n_o + 3 * j
                sg = landed(g)
                su = landed(g + 1)
                a = act_of(hbuf[...], sg, su)
                refill(g, total)
                refill(g + 1, total)
                sd = landed(g + 2)
                yacc[...] += dot32t(a, wbuf[sd])
                refill(g + 2, total)
                return cc
            lax.fori_loop(0, n_f, f_block, 0)
            ysend[k] = (x1buf[...].astype(f32) + yacc[...]).astype(bf16)
            act_copy(k).start()
            return carry
        lax.fori_loop(0, num_k, one_chunk, 0)

    @pl.when(stage == last_stage)
    def _():
        small = x6.shape[0]
        x6[...] = jnp.zeros_like(x6)
        o6[...] = jnp.zeros_like(o6)
        row_id = lax.broadcasted_iota(jnp.int32, (small, q_cols), 0)
        for b in range(n_q + 1):
            landed(b)

        def one_chunk(k, carry):
            wait_x(k)
            hbuf[...] = norm_rows(xin[k].astype(f32), ga_ref[...])
            keys_values(k, 0)
            sel = sel_ref[k]
            x6[...] += dot32(sel, xin[k])
            hsel[...] = dot32(sel, hbuf[...]).astype(bf16)

            def q_block(j, cc):
                v = rope_block(dot32(hsel[...], wbuf[1 + j]), cosl_ref[k], sinl_ref[k])
                for i in range(BLK // 128):
                    qbuf[:small, pl.ds(pl.multiple_of(j * BLK + i * 128, 128), 128)] = (v[i] * scale).astype(bf16)
                return cc
            lax.fori_loop(0, n_q, q_block, 0)
            attend(qbuf.at[:small], obuf.at[:small], maskl_ref.at[k], small)
            o6[...] = jnp.where(row_id // 2 == k, obuf[:small].astype(f32), o6[...])
            return carry
        lax.fori_loop(0, num_k, one_chunk, 0)
        for b in range(n_q + 1):
            refill(b, per)
        o_in = o6[...].astype(bf16)

        def o_block(j, cc):
            g = 1 + n_q + j
            slot = landed(g)
            x1buf[:small, block_at(j)] = (x6[:, block_at(j)] + dot32(o_in, wbuf[slot])).astype(bf16)
            refill(g, per)
            return cc
        lax.fori_loop(0, n_o, o_block, 0)
        x1 = x1buf[:small].astype(f32)
        hsel[...] = norm_rows(x1, gm_ref[...])
        yacc[:small] = jnp.zeros_like(x1)

        def f_block(j, cc):
            g = 1 + n_q + n_o + 3 * j
            sg = landed(g)
            su = landed(g + 1)
            a = act_of(hsel[...], sg, su)
            refill(g, per)
            refill(g + 1, per)
            sd = landed(g + 2)
            yacc[:small] += dot32t(a, wbuf[sd])
            refill(g + 2, per)
            return cc
        lax.fori_loop(0, n_f, f_block, 0)
        rowbuf[...] = (x1buf[:small].astype(f32) + yacc[:small]).astype(bf16)

        def send(d, carry):
            row_copy(d).start()
            return carry
        lax.fori_loop(1, n_dev, send, 0)
        pltpu.make_async_copy(rowbuf, rows_out.at[col], row_self).start()

    def drain(d, carry):
        src = lax.rem(me + d, n_dev)
        for k in range(num_k):
            kv_copy(k, d, me).wait_send()
            kv_copy(k, d, src).wait_recv()
        return carry
    lax.fori_loop(1, n_dev, drain, 0)
    for k in range(num_k):
        kv_local(k).wait()

    @pl.when(lax.rem(col, 2) == 0)
    def _():
        nb_copy().wait_send()

    @pl.when(stage < last_stage)
    def _():
        for k in range(num_k):
            act_copy(k).wait_send()

    @pl.when(stage == last_stage)
    def _():
        def sent(d, carry):
            row_copy(d).wait_send()
            return carry
        lax.fori_loop(1, n_dev, sent, 0)
        pltpu.make_async_copy(rowbuf, rows_out.at[col], row_self).wait()

    for z in range(width):
        @pl.when((stage < last_stage) | (col != z))
        def _():
            row_copy(1, z).wait_recv()


def solution(mesh):
    stages = mesh.shape['model']
    width = mesh.shape['model2']
    stage_spec = P('model', None, None)
    in_specs = (P('replica', None, None, None), P('replica', None), P('replica', None),
                stage_spec, stage_spec, stage_spec, stage_spec, P(None, None), P(None, None),
                P(None, None, TP_AXES, None), P(None, None, TP_AXES, None), P(None, None, TP_AXES, None),
                P(None, TP_AXES, None, None), P(None, None, TP_AXES), P(None, None, TP_AXES), P(None, TP_AXES, None))
    cache_spec = P(None, 'replica', None, TP_AXES, None)
    out_specs = (P('replica', None), P('replica', None), cache_spec, cache_spec)
    num_k = len(CHUNKS)
    pid_tab = np.array([[c[0] for c in row] for row in CHUNKS], np.int32)
    half_tab = np.array([[c[1] for c in row] for row in CHUNKS], np.int32)

    def shard_body(x_prompt, lengths, x_new, st_qkv, st_out, st_gateup, st_down_t, gain_attn, gain_mlp, tp_query, tp_key, tp_value, tp_out, tp_gate, tp_up, tp_down):
        seq_len, model_dim = x_prompt.shape[2:]
        batch = x_new.shape[0]
        head_dim = tp_query.shape[-1]
        w_qkv, w_out, w_gateup, w_down_t = st_qkv[0], st_out[0], st_gateup[0], st_down_t[0]
        q_cols = w_out.shape[0]
        ff = w_down_t.shape[1]
        chunk = seq_len // 2
        rows = chunk + 16
        small = 16
        stage = lax.axis_index('model')
        col = lax.axis_index('model2')
        g_attn = lax.dynamic_slice_in_dim(gain_attn, stage, 1, 0)
        g_mlp = lax.dynamic_slice_in_dim(gain_mlp, stage, 1, 0)
        lens = lengths.reshape(batch)
        x_chunks = x_prompt.reshape(batch, 2, chunk, model_dim)
        pids = jnp.asarray(pid_tab)[:, col]
        halves = jnp.asarray(half_tab)[:, col]
        x_mine = jnp.stack([jnp.concatenate([x_chunks[pids[k], halves[k]], x_new[pids[k]][None], jnp.zeros((rows - chunk - 1, model_dim), jnp.bfloat16)], axis=0)
                            for k in range(num_k)])
        len_k = lens[pids][:, None]
        half_k = halves[:, None]
        row_i = jnp.arange(rows)[None]
        pos = jnp.where(row_i < chunk, half_k * chunk + row_i, len_k)

        def tables(p):
            cos_h, sin_h = rope_angles(p, head_dim)
            return jnp.concatenate([cos_h] * 4, axis=-1), jnp.concatenate([-sin_h, sin_h] * 2, axis=-1)

        def masks(p, dec):
            j = jnp.arange(KEYS)[None, None]
            kpos = jnp.where(j < chunk, j, half_k[..., None] * chunk + j - chunk)
            seen = jnp.where(j < chunk, half_k[..., None] == 1, j < 2 * chunk)
            m = seen & (kpos < len_k[..., None]) & (dec | (kpos <= p[..., None]))
            return (m | (dec & (j == 2 * chunk))).astype(jnp.float32)

        cos_t, sin_t = tables(pos)
        mask = masks(pos, jnp.broadcast_to(row_i >= chunk, pos.shape)[..., None])
        s_i = jnp.arange(small)[None]
        is_dec = jnp.broadcast_to(s_i % 2 == 1, (num_k, small))
        last_i = jnp.clip(len_k - 1 - half_k * chunk, 0, chunk - 1)
        pick = jnp.where(is_dec, chunk, last_i)
        mine = s_i // 2 == jnp.arange(num_k)[:, None]
        sel = (mine[..., None] & (pick[..., None] == row_i[:, None])).astype(jnp.bfloat16)
        pos_l = jnp.where(is_dec, len_k, half_k * chunk + last_i)
        cos_l, sin_l = tables(pos_l)
        mask_l = masks(pos_l, is_dec[..., None])

        dims = (stages, width, num_k, rows, chunk, model_dim, q_cols, ff)
        bf16, f32 = jnp.bfloat16, jnp.float32
        n_dev = stages * width
        vm = pl.BlockSpec(memory_space=pltpu.VMEM)
        hbm = pl.BlockSpec(memory_space=pl.ANY)
        dma = pltpu.SemaphoreType.DMA
        kv_all, rows_all = pl.pallas_call(
            functools.partial(mega_kernel, dims),
            out_shape=(jax.ShapeDtypeStruct((stages, width, num_k, rows, 128), bf16),
                       jax.ShapeDtypeStruct((width, small, model_dim), bf16)),
            in_specs=[hbm] + [vm] * 9 + [hbm] * 4,
            out_specs=(hbm, hbm),
            scratch_shapes=[
                pltpu.VMEM((NBUF, model_dim, BLK), bf16),
                pltpu.VMEM((num_k, rows, model_dim), bf16),
                pltpu.VMEM((num_k, rows, model_dim), bf16),
                pltpu.VMEM((num_k, stages, rows, 128), bf16),
                pltpu.VMEM((stages, rows, 128), bf16),
                pltpu.VMEM((stages, 2 * KEYS, 128), bf16),
                pltpu.VMEM((stages, 2 * KEYS, 128), bf16),
                pltpu.VMEM((rows, q_cols), bf16),
                pltpu.VMEM((rows, q_cols), bf16),
                pltpu.VMEM((rows, model_dim), bf16),
                pltpu.VMEM((rows, model_dim), bf16),
                pltpu.VMEM((rows, model_dim), f32),
                pltpu.VMEM((small, model_dim), bf16),
                pltpu.VMEM((small, model_dim), f32),
                pltpu.VMEM((small, q_cols), f32),
                pltpu.VMEM((small, model_dim), bf16),
                dma((NBUF,)), dma((num_k,)), dma((num_k,)), dma((num_k * n_dev,)), dma((num_k * n_dev,)), dma((num_k,)),
                dma, dma, dma((n_dev,)), dma((width,)), dma,
            ],
            compiler_params=pltpu.CompilerParams(collective_id=0, has_side_effects=True, vmem_limit_bytes=67043328),
            name='pipeline',
        )(x_mine, cos_t, sin_t, mask, sel, cos_l, sin_l, mask_l, g_attn, g_mlp, w_qkv, w_out, w_gateup, w_down_t)

        where_a = {}
        where_b = {}
        for k in range(num_k):
            for z in range(width):
                (where_b if CHUNKS[k][z][1] else where_a)[CHUNKS[k][z][0]] = (z, k)
        dec = jnp.stack([rows_all[where_b[p][0], 2 * where_b[p][1] + 1] for p in range(batch)])
        last = jnp.stack([jnp.where(lens[p] > chunk, rows_all[where_b[p][0], 2 * where_b[p][1]], rows_all[where_a[p][0], 2 * where_a[p][1]])
                          for p in range(batch)])
        full_kv = jnp.stack([jnp.concatenate([kv_all[:, where_a[p][0], where_a[p][1], :chunk],
                                              kv_all[:, where_b[p][0], where_b[p][1], :chunk + 1]], axis=1)
                             for p in range(batch)], axis=1)
        k_full = full_kv[:, :, :, None, :head_dim]
        v_full = full_kv[:, :, :, None, head_dim:]
        return dec, last, k_full, v_full

    return jax.shard_map(shard_body, mesh=mesh, in_specs=in_specs, out_specs=out_specs, check_vma=False)
```

```python
import functools

import jax
import jax.numpy as jnp
import numpy as np
from jax import lax
from jax.experimental import pallas as pl
from jax.experimental.pallas import tpu as pltpu
from jax.sharding import PartitionSpec as P

EPS = 1e-5
THETA = 10000.0
TP_AXES = ('model', 'model2')
NEG = -1e30
BLK = 512
NBUF = 18
KEYS = 512
MESH_ID = pl.DeviceIdType.MESH

CHUNKS = (((4, 0), (1, 0), (5, 0), (3, 0)),
          ((0, 0), (1, 1), (2, 0), (3, 1)),
          ((0, 1), (4, 1), (2, 1), (5, 1)))


def dot32(a, b):
    return jnp.dot(a, b, preferred_element_type=jnp.float32)


def dot32t(a, b):
    return lax.dot_general(a, b, (((1,), (1,)), ((), ())), preferred_element_type=jnp.float32)


def norm_rows(x_f32, gain):
    inv_rms = lax.rsqrt(jnp.mean(x_f32 * x_f32, axis=-1, keepdims=True) + EPS)
    return (x_f32 * inv_rms * gain).astype(jnp.bfloat16)


def rope_block(v, cos_t, sin_t):
    lane = lax.broadcasted_iota(jnp.int32, (v.shape[0], 128), 1)
    first = (lane % 64) < 32
    out = []
    for c in range(v.shape[1] // 128):
        t = v[:, c * 128:(c + 1) * 128]
        other = jnp.where(first, pltpu.roll(t, 96, 1), pltpu.roll(t, 32, 1))
        out.append(t * cos_t + other * sin_t)
    return out


def mega_kernel(dims, lens, x_prompt, x_new, tab_cos, tab_sin, ga_all, gm_all,
                w_qkv, w_out, w_gu, w_dt, kv_out, dec_out, last_out,
                wbuf, xin, ysend, kvst, nb, kst, vst, qbuf, obuf, hbuf, x1buf, yacc, cosb, sinb, maskb, coslb, sinlb, masklb,
                hsel, x6, o6, hg, yparts, yrecv, rowbuf, rland,
                wsem, act_send, act_recv, kv_send, kv_recv, kv_self, nb_send, nb_recv, row_send, row_recv,
                h_send, h_recv, p_send, p_recv):
    stages, width, num_k, rows, chunk, model_dim, q_cols, ff = dims
    n_dev = stages * width
    n_q = q_cols // BLK
    n_o = model_dim // BLK
    n_f = ff // BLK
    per = n_q + 1 + n_o + 3 * n_f
    stage = lax.axis_index('model')
    col = lax.axis_index('model2')
    me = stage * width + col
    last_stage = stages - 1
    f32 = jnp.float32
    bf16 = jnp.bfloat16
    small = x6.shape[0]
    row_count = x_prompt.shape[1]
    ga_ref = ga_all.at[pl.ds(stage, 1)]
    gm_ref = gm_all.at[pl.ds(stage, 1)]

    def here(k, table):
        out = table[0][0]
        for kk in range(num_k):
            for z in range(width):
                out = jnp.where((k == kk) & (col == z), table[kk][z], out)
        return out

    len_tab = [[lens[p // row_count, p % row_count] for p, _ in line] for line in CHUNKS]
    half_tab = [[h for _, h in line] for line in CHUNKS]

    def iota(shape, dim):
        return lax.broadcasted_iota(jnp.int32, shape, dim)

    def visible(j, pos, dec, length, half):
        kpos = jnp.where(j < chunk, j, half * chunk + j - chunk)
        seen = (j >= chunk * (1 - half)) & (j < 2 * chunk) & (kpos < length) & (dec | (kpos <= pos))
        return jnp.where(seen | (dec & (j == 2 * chunk)), 1.0, 0.0)

    def set_tables(k):
        length, half = here(k, len_tab), here(k, half_tab)
        at = pl.ds(pl.multiple_of(half * chunk, 8), chunk)
        t_i = iota(tab_cos.shape, 0)
        odd = iota((small, 128), 0) % 2 == 1
        for tab, buf, buf_l in ((tab_cos, cosb, coslb), (tab_sin, sinb, sinlb)):
            buf[:chunk] = tab[at, :]
            at_len = jnp.sum(jnp.where(t_i == length, tab[...], 0.0), axis=0, keepdims=True)
            buf[chunk:] = jnp.broadcast_to(at_len, (rows - chunk, 128))

            @pl.when(stage == last_stage)
            def _():
                at_last = jnp.sum(jnp.where(t_i == length - 1, tab[...], 0.0), axis=0, keepdims=True)
                buf_l[...] = jnp.where(odd, at_len, at_last)

        @pl.when(stage < last_stage)
        def _():
            i = iota((rows, KEYS), 0)
            dec = i >= chunk
            maskb[...] = visible(iota((rows, KEYS), 1), jnp.where(dec, length, half * chunk + i), dec, length, half)

        @pl.when(stage == last_stage)
        def _():
            dec = iota((small, KEYS), 0) % 2 == 1
            masklb[...] = visible(iota((small, KEYS), 1), jnp.where(dec, length, length - 1), dec, length, half)

    def wslot(g):
        return lax.rem(g, NBUF)

    def fetch(g):
        b = lax.rem(g, per)
        slot = wslot(g)

        def go(src, j):
            pltpu.make_async_copy(src.at[:, pl.ds(pl.multiple_of(j * BLK, BLK), BLK)], wbuf.at[slot], wsem.at[slot]).start()

        @pl.when(b == 0)
        def _():
            go(w_qkv, n_q)

        @pl.when((b >= 1) & (b <= n_q))
        def _():
            go(w_qkv, b - 1)

        @pl.when((b > n_q) & (b <= n_q + n_o))
        def _():
            go(w_out, b - n_q - 1)

        f = b - (n_q + n_o + 1)

        @pl.when((f >= 0) & (lax.rem(f, 3) == 0))
        def _():
            go(w_gu, f // 3)

        @pl.when((f >= 0) & (lax.rem(f, 3) == 1))
        def _():
            go(w_gu, n_f + f // 3)

        @pl.when((f >= 0) & (lax.rem(f, 3) == 2))
        def _():
            go(w_dt, f // 3)

    def fetch_last(b):
        def go(src, j):
            pltpu.make_async_copy(src.at[:, pl.ds(pl.multiple_of(j * BLK, BLK), BLK)], wbuf.at[b], wsem.at[b]).start()
        if b == 0:
            go(w_qkv, n_q)
        elif b <= n_q:
            go(w_qkv, b - 1)
        elif b <= n_q + n_o:
            go(w_out, b - n_q - 1)
        else:
            i = b - (n_q + n_o + 1)
            j = lax.min(col + (i // 3) * width, n_f - 1)
            if i % 3 == 0:
                go(w_gu, j)
            elif i % 3 == 1:
                go(w_gu, n_f + j)
            else:
                go(w_dt, j)

    def landed(g):
        slot = wslot(g)
        pltpu.make_async_copy(w_out.at[:, pl.ds(0, BLK)], wbuf.at[slot], wsem.at[slot]).wait()
        return slot

    def refill(g, total):
        @pl.when(g + NBUF < total)
        def _():
            fetch(g + NBUF)

    def first_fetch(g, carry):
        fetch(g)
        return carry
    n_mine = (n_f + width - 1) // width
    n_last = n_q + 1 + n_o + 3 * n_mine

    def x_copy(k, z):
        p, h = CHUNKS[k][z]
        return pltpu.make_async_copy(x_prompt.at[p // row_count, p % row_count, pl.ds(h * chunk, chunk)], xin.at[k, pl.ds(0, chunk)], act_recv.at[k])

    @pl.when(stage == 0)
    def _():
        for z in range(width):
            @pl.when(col == z)
            def _():
                for k in range(num_k):
                    x_copy(k, z).start()

    @pl.when(stage < last_stage)
    def _():
        lax.fori_loop(0, NBUF, first_fetch, 0)

    @pl.when(stage == last_stage)
    def _():
        for b in range(n_last):
            fetch_last(b)

    barrier = pltpu.get_barrier_semaphore()

    def peer(d):
        t = lax.rem(me + d, n_dev)
        return t // width, lax.rem(t, width)

    def greet(d, carry):
        c, z = peer(d)
        pl.semaphore_signal(barrier, inc=1, device_id={'model': c, 'model2': z}, device_id_type=MESH_ID)
        return carry
    lax.fori_loop(1, n_dev, greet, 0)

    @pl.when(stage == 0)
    def _():
        for z in range(width):
            @pl.when(col == z)
            def _():
                for k in range(num_k):
                    p = CHUNKS[k][z][0]
                    new_row = jnp.broadcast_to(x_new[p:p + 1, :].astype(f32), (rows - chunk, model_dim))
                    xin[k, chunk:] = jnp.where(iota(new_row.shape, 0) == 0, new_row, 0.0).astype(bf16)

    kst[...] = jnp.zeros_like(kst)
    vst[...] = jnp.zeros_like(vst)

    def wait_x(k):
        @pl.when(stage == 0)
        def _():
            pltpu.make_async_copy(x_prompt.at[0, 0, pl.ds(0, chunk)], xin.at[k, pl.ds(0, chunk)], act_recv.at[k]).wait()

        @pl.when(stage > 0)
        def _():
            act_copy(k).wait_recv()

    def act_copy(k):
        return pltpu.make_async_remote_copy(src_ref=ysend.at[k], dst_ref=xin.at[k], send_sem=act_send.at[k], recv_sem=act_recv.at[k],
                                            device_id={'model': lax.rem(stage + 1, stages)}, device_id_type=MESH_ID)

    def kv_copy(k, d, src_dev):
        c, z = peer(d)
        return pltpu.make_async_remote_copy(src_ref=kvst.at[k, c], dst_ref=kv_out.at[src_dev // width, lax.rem(src_dev, width), k],
                                            send_sem=kv_send.at[k * n_dev + d], recv_sem=kv_recv.at[src_dev * num_k + k],
                                            device_id={'model': c, 'model2': z}, device_id_type=MESH_ID)

    def kv_local(k):
        return pltpu.make_async_copy(kvst.at[k, stage], kv_out.at[stage, col, k], kv_self.at[k])

    def nb_copy():
        return pltpu.make_async_remote_copy(src_ref=kvst.at[0], dst_ref=nb, send_sem=nb_send, recv_sem=nb_recv,
                                            device_id={'model2': lax.rem(col + 1, width)}, device_id_type=MESH_ID)

    def row_copy(d, src_col):
        c, z = peer(d)
        return pltpu.make_async_remote_copy(src_ref=rowbuf, dst_ref=rland.at[src_col], send_sem=row_send.at[d], recv_sem=row_recv.at[src_col],
                                            device_id={'model': c, 'model2': z}, device_id_type=MESH_ID)

    def h_copy(d, src_col):
        return pltpu.make_async_remote_copy(src_ref=hsel, dst_ref=hg.at[src_col], send_sem=h_send.at[d], recv_sem=h_recv.at[src_col],
                                            device_id={'model2': lax.rem(col + d, width)}, device_id_type=MESH_ID)

    def p_copy(d, src_col):
        z = lax.rem(col + d, width)
        return pltpu.make_async_remote_copy(src_ref=yparts.at[z], dst_ref=yrecv.at[src_col], send_sem=p_send.at[d], recv_sem=p_recv.at[src_col],
                                            device_id={'model2': z}, device_id_type=MESH_ID)

    lane_r = lax.broadcasted_iota(jnp.int32, (rows, 128), 1)
    low = lane_r < 64

    def stack(c, base, packed):
        n = packed.shape[0]
        lo = low[:n]
        turned = pltpu.roll(packed, 64, 1)
        zero = jnp.zeros_like(packed)
        kst[c, base:base + n, :] = jnp.where(lo, packed, zero).astype(bf16)
        kst[c, KEYS + base:KEYS + base + n, :] = jnp.where(lo, zero, turned).astype(bf16)
        vst[c, base:base + n, :] = jnp.where(lo, turned, zero).astype(bf16)
        vst[c, KEYS + base:KEYS + base + n, :] = jnp.where(lo, zero, packed).astype(bf16)

    def keys_values(k, slot):
        kv = dot32(hbuf[...], wbuf[slot])
        half = kv.shape[1] // 2
        keys = rope_block(kv[:, :half], cosb[...], sinb[...])
        for c in range(stages):
            kt = keys[c // 2]
            vt = kv[:, half + (c // 2) * 128:half + (c // 2 + 1) * 128]
            if c % 2 == 0:
                packed = jnp.where(low, kt, pltpu.roll(vt, 64, 1))
            else:
                packed = jnp.where(low, pltpu.roll(kt, 64, 1), vt)
            packed = packed.astype(bf16)
            kvst[k, c] = packed
            stack(c, chunk, packed.astype(f32))

        @pl.when(k == 0)
        def _():
            pl.semaphore_wait(barrier, n_dev - 1)

            @pl.when(lax.rem(col, 2) == 0)
            def _():
                nb_copy().start()

        kv_local(k).start()

        use_nb = (k == num_k - 1) & (lax.rem(col, 2) == 1)

        @pl.when(use_nb)
        def _():
            nb_copy().wait_recv()
            for c in range(stages):
                stack(c, 0, nb[c, :chunk].astype(f32))

        @pl.when((k > 0) & jnp.logical_not(use_nb))
        def _():
            for c in range(stages):
                stack(c, 0, kvst[lax.max(k - 1, 0), c, :chunk].astype(f32))

    def attend(q_ref, o_ref, m_ref, n_rows):
        pairs = q_cols // 128
        per_c = pairs // stages

        def pair(i, carry):
            c = i // per_c
            at = pl.ds(pl.multiple_of(i * 128, 128), 128)
            s = dot32t(q_ref[:, at], kst[c])
            parts = []
            for e in range(2):
                se = jnp.where(m_ref[...] > 0.5, s[:, e * KEYS:(e + 1) * KEYS], NEG)
                ex = jnp.exp(se - jnp.max(se, axis=-1, keepdims=True))
                inv = 1.0 / jnp.sum(ex, axis=-1, keepdims=True)
                parts.append((ex * inv).astype(bf16))
            o_ref[:, at] = dot32(jnp.concatenate(parts, axis=1), vst[c]).astype(bf16)
            return carry
        lax.fori_loop(0, pairs, pair, 0)

    scale = 64 ** -0.5

    def block_at(j):
        return pl.ds(pl.multiple_of(j * BLK, BLK), BLK)

    def act_of(h, slot_g, slot_u):
        g = dot32(h, wbuf[slot_g])
        u = dot32(h, wbuf[slot_u])
        return (g * jax.nn.sigmoid(g) * u).astype(bf16)

    @pl.when(stage < last_stage)
    def _():
        total = per * num_k

        def one_chunk(k, carry):
            g0 = k * per
            set_tables(k)
            wait_x(k)
            hbuf[...] = norm_rows(xin[k].astype(f32), ga_ref[...])
            keys_values(k, landed(g0))
            refill(g0, total)

            def q_block(j, cc):
                g = g0 + 1 + j
                slot = landed(g)
                v = rope_block(dot32(hbuf[...], wbuf[slot]), cosb[...], sinb[...])
                for i in range(BLK // 128):
                    qbuf[:, pl.ds(pl.multiple_of(j * BLK + i * 128, 128), 128)] = (v[i] * scale).astype(bf16)
                refill(g, total)
                return cc
            lax.fori_loop(0, n_q, q_block, 0)

            attend(qbuf, obuf, maskb, rows)

            def o_block(j, cc):
                g = g0 + 1 + n_q + j
                slot = landed(g)
                kv_copy(k, 1 + j, me).start()
                x1buf[:, block_at(j)] = (xin[k, :, block_at(j)].astype(f32) + dot32(obuf[...], wbuf[slot])).astype(bf16)
                refill(g, total)
                return cc
            lax.fori_loop(0, n_o, o_block, 0)

            x1 = x1buf[...].astype(f32)
            hbuf[...] = norm_rows(x1, gm_ref[...])
            yacc[...] = jnp.zeros_like(yacc)

            def f_block(j, cc):
                g = g0 + 1 + n_q + n_o + 3 * j
                sg = landed(g)
                su = landed(g + 1)
                kv_copy(k, 1 + n_o + j, me).start()
                a = act_of(hbuf[...], sg, su)
                refill(g, total)
                refill(g + 1, total)
                sd = landed(g + 2)
                yacc[...] += dot32t(a, wbuf[sd])
                refill(g + 2, total)
                return cc
            lax.fori_loop(0, n_f, f_block, 0)
            ysend[k] = (x1buf[...].astype(f32) + yacc[...]).astype(bf16)
            act_copy(k).start()
            return carry
        lax.fori_loop(0, num_k, one_chunk, 0)

    @pl.when(stage == last_stage)
    def _():
        x6[...] = jnp.zeros_like(x6)
        o6[...] = jnp.zeros_like(o6)
        row_id = iota((small, q_cols), 0)
        for b in range(n_q + 1):
            landed(b)

        def one_chunk(k, carry):
            set_tables(k)
            wait_x(k)
            hbuf[...] = norm_rows(xin[k].astype(f32), ga_ref[...])
            keys_values(k, 0)

            def send(d, cc):
                kv_copy(k, d, me).start()
                return cc
            lax.fori_loop(1, n_dev, send, 0)
            r = iota((small, rows), 0)
            last_i = lax.clamp(0, here(k, len_tab) - 1 - here(k, half_tab) * chunk, chunk - 1)
            pick = jnp.where(r % 2 == 1, chunk, last_i)
            sel = jnp.where((r // 2 == k) & (iota((small, rows), 1) == pick), 1.0, 0.0).astype(bf16)
            x6[...] += dot32(sel, xin[k])
            hs = dot32(sel, hbuf[...]).astype(bf16)

            def q_block(j, cc):
                v = rope_block(dot32(hs, wbuf[1 + j]), coslb[...], sinlb[...])
                for i in range(BLK // 128):
                    qbuf[:small, pl.ds(pl.multiple_of(j * BLK + i * 128, 128), 128)] = (v[i] * scale).astype(bf16)
                return cc
            lax.fori_loop(0, n_q, q_block, 0)
            attend(qbuf.at[:small], obuf.at[:small], masklb, small)
            o6[...] = jnp.where(row_id // 2 == k, obuf[:small].astype(f32), o6[...])
            return carry
        lax.fori_loop(0, num_k, one_chunk, 0)
        for b in range(n_q + 1, n_last):
            landed(b)
        o_in = o6[...].astype(bf16)

        def o_block(j, cc):
            x1buf[:small, block_at(j)] = (x6[:, block_at(j)] + dot32(o_in, wbuf[1 + n_q + j])).astype(bf16)
            return cc
        lax.fori_loop(0, n_o, o_block, 0)
        x1 = x1buf[:small].astype(f32)
        hsel[...] = norm_rows(x1, gm_ref[...])
        for d in range(1, width):
            h_copy(d, col).start()
        hg[col] = hsel[...]
        for d in range(1, width):
            h_copy(d, lax.rem(col + d, width)).wait_recv()
        h_all = jnp.concatenate([hg[z].astype(f32) for z in range(width)], axis=0).astype(bf16)
        yacc[:width * small] = jnp.zeros((width * small, model_dim), f32)

        def f_block(i, cc):
            b = 1 + n_q + n_o + 3 * i

            @pl.when(col + width * i < n_f)
            def _():
                yacc[:width * small] += dot32t(act_of(h_all, b, b + 1), wbuf[b + 2])
            return cc
        lax.fori_loop(0, n_mine, f_block, 0)
        for z in range(width):
            yparts[z] = yacc[z * small:(z + 1) * small]
        for d in range(1, width):
            p_copy(d, col).start()
        yrecv[col] = yparts[col]
        for d in range(1, width):
            p_copy(d, lax.rem(col + d, width)).wait_recv()
        rowbuf[...] = (x1 + (yrecv[0] + yrecv[1] + yrecv[2] + yrecv[3])).astype(bf16)

        def send(d, carry):
            row_copy(d, col).start()
            return carry
        lax.fori_loop(1, n_dev, send, 0)
        rland[col] = rowbuf[...]

    def drain(d, carry):
        src = lax.rem(me + d, n_dev)
        for k in range(num_k):
            kv_copy(k, d, me).wait_send()
            kv_copy(k, d, src).wait_recv()
        return carry
    lax.fori_loop(1, n_dev, drain, 0)
    for k in range(num_k):
        kv_local(k).wait()

    @pl.when(lax.rem(col, 2) == 0)
    def _():
        nb_copy().wait_send()

    @pl.when(stage < last_stage)
    def _():
        for k in range(num_k):
            act_copy(k).wait_send()

    @pl.when(stage == last_stage)
    def _():
        for d in range(1, width):
            h_copy(d, col).wait_send()
            p_copy(d, col).wait_send()

        def sent(d, carry):
            row_copy(d, col).wait_send()
            return carry
        lax.fori_loop(1, n_dev, sent, 0)

    for z in range(width):
        @pl.when((stage < last_stage) | (col != z))
        def _():
            row_copy(1, z).wait_recv()

    first, second = {}, {}
    for k in range(num_k):
        for z in range(width):
            (second if CHUNKS[k][z][1] else first)[CHUNKS[k][z][0]] = (z, k)
    got = [rland[z].astype(f32) for z in range(width)]

    def row_of(place, odd):
        return got[place[0]][2 * place[1] + odd:2 * place[1] + odd + 1]
    batch = dec_out.shape[0]
    dec_out[...] = jnp.concatenate([row_of(second[p], 1) for p in range(batch)], axis=0).astype(bf16)
    last_out[...] = jnp.concatenate([jnp.where(lens[p // row_count, p % row_count] > chunk, row_of(second[p], 0), row_of(first[p], 0))
                                     for p in range(batch)], axis=0).astype(bf16)


def solution(mesh):
    stages = mesh.shape['model']
    width = mesh.shape['model2']
    stage_spec = P('model', None, None)
    in_specs = (P('replica', None, None, None), P('replica', None), P('replica', None),
                stage_spec, stage_spec, stage_spec, stage_spec, P(None, None), P(None, None),
                P(None, None, TP_AXES, None), P(None, None, TP_AXES, None), P(None, None, TP_AXES, None),
                P(None, TP_AXES, None, None), P(None, None, TP_AXES), P(None, None, TP_AXES), P(None, TP_AXES, None))
    cache_spec = P(None, 'replica', None, TP_AXES, None)
    out_specs = (P('replica', None), P('replica', None), cache_spec, cache_spec)
    num_k = len(CHUNKS)
    def shard_body(x_prompt, lengths, x_new, st_qkv, st_out, st_gateup, st_down_t, gain_attn, gain_mlp, tp_query, tp_key, tp_value, tp_out, tp_gate, tp_up, tp_down):
        seq_len, model_dim = x_prompt.shape[2:]
        batch = x_new.shape[0]
        head_dim = tp_query.shape[-1]
        w_qkv, w_out, w_gateup, w_down_t = st_qkv[0], st_out[0], st_gateup[0], st_down_t[0]
        q_cols = w_out.shape[0]
        ff = w_down_t.shape[1]
        chunk = seq_len // 2
        rows = chunk + 16
        small = 8
        half_dim = head_dim // 2
        inv_freq = np.power(np.float32(THETA), np.arange(half_dim, dtype=np.float32) * np.float32(-2.0 / head_dim)).astype(np.float32)
        angles = (np.arange(seq_len + 8, dtype=np.float32)[:, None] * inv_freq).astype(np.float32)
        cos_h, sin_h = np.cos(angles).astype(np.float32), np.sin(angles).astype(np.float32)
        tab_cos = jnp.asarray(np.concatenate([cos_h] * 4, axis=1))
        tab_sin = jnp.asarray(np.concatenate([-sin_h, sin_h] * 2, axis=1))

        dims = (stages, width, num_k, rows, chunk, model_dim, q_cols, ff)
        bf16, f32 = jnp.bfloat16, jnp.float32
        n_dev = stages * width
        vm = pl.BlockSpec(memory_space=pltpu.VMEM)
        hbm = pl.BlockSpec(memory_space=pl.ANY)
        dma = pltpu.SemaphoreType.DMA
        kv_all, dec, last = pl.pallas_call(
            functools.partial(mega_kernel, dims),
            out_shape=(jax.ShapeDtypeStruct((stages, width, num_k, rows, 128), bf16),
                       jax.ShapeDtypeStruct((batch, model_dim), bf16), jax.ShapeDtypeStruct((batch, model_dim), bf16)),
            in_specs=[pl.BlockSpec(memory_space=pltpu.SMEM), hbm] + [vm] * 5 + [hbm] * 4,
            out_specs=(hbm, vm, vm),
            scratch_shapes=[
                pltpu.VMEM((NBUF, model_dim, BLK), bf16),
                pltpu.VMEM((num_k, rows, model_dim), bf16),
                pltpu.VMEM((num_k, rows, model_dim), bf16),
                pltpu.VMEM((num_k, stages, rows, 128), bf16),
                pltpu.VMEM((stages, rows, 128), bf16),
                pltpu.VMEM((stages, 2 * KEYS, 128), bf16),
                pltpu.VMEM((stages, 2 * KEYS, 128), bf16),
                pltpu.VMEM((rows, q_cols), bf16),
                pltpu.VMEM((rows, q_cols), bf16),
                pltpu.VMEM((rows, model_dim), bf16),
                pltpu.VMEM((rows, model_dim), bf16),
                pltpu.VMEM((rows, model_dim), f32),
                pltpu.VMEM((rows, 128), f32),
                pltpu.VMEM((rows, 128), f32),
                pltpu.VMEM((rows, KEYS), f32),
                pltpu.VMEM((small, 128), f32),
                pltpu.VMEM((small, 128), f32),
                pltpu.VMEM((small, KEYS), f32),
                pltpu.VMEM((small, model_dim), bf16),
                pltpu.VMEM((small, model_dim), f32),
                pltpu.VMEM((small, q_cols), f32),
                pltpu.VMEM((width, small, model_dim), bf16),
                pltpu.VMEM((width, small, model_dim), f32),
                pltpu.VMEM((width, small, model_dim), f32),
                pltpu.VMEM((small, model_dim), bf16),
                pltpu.VMEM((width, small, model_dim), bf16),
                dma((NBUF,)), dma((num_k,)), dma((num_k,)), dma((num_k * n_dev,)), dma((num_k * n_dev,)), dma((num_k,)),
                dma, dma, dma((n_dev,)), dma((width,)), dma((width,)), dma((width,)), dma((width,)), dma((width,)),
            ],
            compiler_params=pltpu.CompilerParams(collective_id=0, has_side_effects=True, vmem_limit_bytes=67043328),
            name='pipeline',
        )(lengths, x_prompt, x_new, tab_cos, tab_sin, gain_attn, gain_mlp, w_qkv, w_out, w_gateup, w_down_t)

        where_a = {}
        where_b = {}
        for k in range(num_k):
            for z in range(width):
                (where_b if CHUNKS[k][z][1] else where_a)[CHUNKS[k][z][0]] = (z, k)
        full_kv = jnp.stack([jnp.concatenate([kv_all[:, where_a[p][0], where_a[p][1], :chunk],
                                              kv_all[:, where_b[p][0], where_b[p][1], :chunk + 1]], axis=1)
                             for p in range(batch)], axis=1)
        k_full = full_kv[:, :, :, None, :head_dim]
        v_full = full_kv[:, :, :, None, head_dim:]
        return dec, last, k_full, v_full

    return jax.shard_map(shard_body, mesh=mesh, in_specs=in_specs, out_specs=out_specs, check_vma=False)
```

```python
import functools

import jax
import jax.numpy as jnp
import numpy as np
from jax import lax
from jax.experimental import pallas as pl
from jax.experimental.pallas import tpu as pltpu
from jax.sharding import PartitionSpec as P

EPS = 1e-5
THETA = 10000.0
TP_AXES = ('model', 'model2')
NEG = -1e30
BLK = 512
NBUF = 18
KEYS = 512
MESH_ID = pl.DeviceIdType.MESH

CHUNKS = (((4, 0), (1, 0), (5, 0), (3, 0)),
          ((0, 0), (1, 1), (2, 0), (3, 1)),
          ((0, 1), (4, 1), (2, 1), (5, 1)))


def dot32(a, b):
    return jnp.dot(a, b, preferred_element_type=jnp.float32)


def dot32t(a, b):
    return lax.dot_general(a, b, (((1,), (1,)), ((), ())), preferred_element_type=jnp.float32)


def norm_rows(x_f32, gain):
    inv_rms = lax.rsqrt(jnp.mean(x_f32 * x_f32, axis=-1, keepdims=True) + EPS)
    return (x_f32 * inv_rms * gain).astype(jnp.bfloat16)


def rope_block(v, cos_t, sin_t):
    lane = lax.broadcasted_iota(jnp.int32, (v.shape[0], 128), 1)
    first = (lane % 64) < 32
    out = []
    for c in range(v.shape[1] // 128):
        t = v[:, c * 128:(c + 1) * 128]
        other = jnp.where(first, pltpu.roll(t, 96, 1), pltpu.roll(t, 32, 1))
        out.append(t * cos_t + other * sin_t)
    return out


def mega_kernel(dims, lens, x_prompt, x_new, tab_cos, tab_sin, ga_all, gm_all,
                w_qkv, w_out, w_gu, w_dt, kv_out, dec_out, last_out,
                wbuf, xin, ysend, kvst, nb, kst, vst, qbuf, obuf, hbuf, x1buf, yacc, abuf, cosb, sinb, maskb, coslb, sinlb, masklb,
                hsel, x6, o6, hg, yparts, yrecv, rowbuf, rland,
                wsem, act_send, act_recv, kv_send, kv_recv, kv_self, nb_send, nb_recv, row_send, row_recv,
                h_send, h_recv, p_send, p_recv):
    stages, width, num_k, rows, chunk, model_dim, q_cols, ff = dims
    n_dev = stages * width
    n_q = q_cols // BLK
    n_o = model_dim // BLK
    n_f = ff // BLK
    per = n_q + 1 + n_o + 3 * n_f
    stage = lax.axis_index('model')
    col = lax.axis_index('model2')
    me = stage * width + col
    last_stage = stages - 1
    f32 = jnp.float32
    bf16 = jnp.bfloat16
    small = x6.shape[0]
    row_count = x_prompt.shape[1]
    ga_ref = ga_all.at[pl.ds(stage, 1)]
    gm_ref = gm_all.at[pl.ds(stage, 1)]

    def here(k, table):
        out = table[0][0]
        for kk in range(num_k):
            for z in range(width):
                out = jnp.where((k == kk) & (col == z), table[kk][z], out)
        return out

    len_tab = [[lens[p // row_count, p % row_count] for p, _ in line] for line in CHUNKS]
    half_tab = [[h for _, h in line] for line in CHUNKS]

    def iota(shape, dim):
        return lax.broadcasted_iota(jnp.int32, shape, dim)

    def visible(j, pos, dec, length, half):
        ctx = KEYS // 2
        kpos = jnp.where(j < ctx, half * chunk + j, j - ctx)
        there = (j < chunk) | ((j >= ctx) & (j < ctx + half * chunk))
        seen = there & (kpos < length) & (dec | (kpos <= pos))
        return jnp.where(seen | (dec & (j == chunk)), 1.0, 0.0)

    def set_tables(k):
        length, half = here(k, len_tab), here(k, half_tab)
        at = pl.ds(pl.multiple_of(half * chunk, 8), chunk)
        t_i = iota(tab_cos.shape, 0)
        odd = iota((small, 128), 0) % 2 == 1
        for tab, buf, buf_l in ((tab_cos, cosb, coslb), (tab_sin, sinb, sinlb)):
            buf[:chunk] = tab[at, :]
            at_len = jnp.sum(jnp.where(t_i == length, tab[...], 0.0), axis=0, keepdims=True)
            buf[chunk:] = jnp.broadcast_to(at_len, (rows - chunk, 128))

            @pl.when(stage == last_stage)
            def _():
                at_last = jnp.sum(jnp.where(t_i == length - 1, tab[...], 0.0), axis=0, keepdims=True)
                buf_l[...] = jnp.where(odd, at_len, at_last)

        @pl.when(stage < last_stage)
        def _():
            i = iota((rows, KEYS), 0)
            dec = i >= chunk
            maskb[...] = visible(iota((rows, KEYS), 1), jnp.where(dec, length, half * chunk + i), dec, length, half)

        @pl.when(stage == last_stage)
        def _():
            dec = iota((small, KEYS), 0) % 2 == 1
            masklb[...] = visible(iota((small, KEYS), 1), jnp.where(dec, length, length - 1), dec, length, half)

    def wslot(g):
        return lax.rem(g, NBUF)

    def fetch(g):
        b = lax.rem(g, per)
        slot = wslot(g)

        def go(src, j):
            pltpu.make_async_copy(src.at[:, pl.ds(pl.multiple_of(j * BLK, BLK), BLK)], wbuf.at[slot], wsem.at[slot]).start()

        @pl.when(b == 0)
        def _():
            go(w_qkv, n_q)

        @pl.when((b >= 1) & (b <= n_q))
        def _():
            go(w_qkv, b - 1)

        @pl.when((b > n_q) & (b <= n_q + n_o))
        def _():
            go(w_out, b - n_q - 1)

        f = b - (n_q + n_o + 1)

        @pl.when((f >= 0) & (lax.rem(f, 3) == 0))
        def _():
            go(w_gu, f // 3)

        @pl.when((f >= 0) & (lax.rem(f, 3) == 1))
        def _():
            go(w_gu, n_f + f // 3)

        @pl.when((f >= 0) & (lax.rem(f, 3) == 2))
        def _():
            go(w_dt, f // 3)

    def fetch_last(b):
        def go(src, j):
            pltpu.make_async_copy(src.at[:, pl.ds(pl.multiple_of(j * BLK, BLK), BLK)], wbuf.at[b], wsem.at[b]).start()
        if b == 0:
            go(w_qkv, n_q)
        elif b <= n_q:
            go(w_qkv, b - 1)
        elif b <= n_q + n_o:
            go(w_out, b - n_q - 1)
        else:
            i = b - (n_q + n_o + 1)
            j = lax.min(col + (i // 3) * width, n_f - 1)
            if i % 3 == 0:
                go(w_gu, j)
            elif i % 3 == 1:
                go(w_gu, n_f + j)
            else:
                go(w_dt, j)

    def landed(g):
        slot = wslot(g)
        pltpu.make_async_copy(w_out.at[:, pl.ds(0, BLK)], wbuf.at[slot], wsem.at[slot]).wait()
        return slot

    def refill(g, total):
        @pl.when(g + NBUF < total)
        def _():
            fetch(g + NBUF)

    def first_fetch(g, carry):
        fetch(g)
        return carry
    n_mine = (n_f + width - 1) // width
    n_last = n_q + 1 + n_o + 3 * n_mine

    def x_copy(k, z):
        p, h = CHUNKS[k][z]
        return pltpu.make_async_copy(x_prompt.at[p // row_count, p % row_count, pl.ds(h * chunk, chunk)], xin.at[k, pl.ds(0, chunk)], act_recv.at[k])

    @pl.when(stage == 0)
    def _():
        for z in range(width):
            @pl.when(col == z)
            def _():
                for k in range(num_k):
                    x_copy(k, z).start()

    @pl.when(stage < last_stage)
    def _():
        lax.fori_loop(0, NBUF, first_fetch, 0)

    @pl.when(stage == last_stage)
    def _():
        for b in range(n_last):
            fetch_last(b)

    barrier = pltpu.get_barrier_semaphore()

    def peer(d):
        t = lax.rem(me + d, n_dev)
        return t // width, lax.rem(t, width)

    def greet(d, carry):
        c, z = peer(d)
        pl.semaphore_signal(barrier, inc=1, device_id={'model': c, 'model2': z}, device_id_type=MESH_ID)
        return carry
    lax.fori_loop(1, n_dev, greet, 0)

    @pl.when(stage == 0)
    def _():
        for z in range(width):
            @pl.when(col == z)
            def _():
                for k in range(num_k):
                    p = CHUNKS[k][z][0]
                    new_row = jnp.broadcast_to(x_new[p:p + 1, :].astype(f32), (rows - chunk, model_dim))
                    xin[k, chunk:] = jnp.where(iota(new_row.shape, 0) == 0, new_row, 0.0).astype(bf16)

    kst[...] = jnp.zeros_like(kst)
    vst[...] = jnp.zeros_like(vst)

    def wait_x(k):
        @pl.when(stage == 0)
        def _():
            pltpu.make_async_copy(x_prompt.at[0, 0, pl.ds(0, chunk)], xin.at[k, pl.ds(0, chunk)], act_recv.at[k]).wait()

        @pl.when(stage > 0)
        def _():
            act_copy(k).wait_recv()

    def act_copy(k):
        return pltpu.make_async_remote_copy(src_ref=ysend.at[k], dst_ref=xin.at[k], send_sem=act_send.at[k], recv_sem=act_recv.at[k],
                                            device_id={'model': lax.rem(stage + 1, stages)}, device_id_type=MESH_ID)

    def kv_copy(k, d, src_dev):
        c, z = peer(d)
        return pltpu.make_async_remote_copy(src_ref=kvst.at[k, c], dst_ref=kv_out.at[src_dev // width, lax.rem(src_dev, width), k],
                                            send_sem=kv_send.at[k * n_dev + d], recv_sem=kv_recv.at[src_dev * num_k + k],
                                            device_id={'model': c, 'model2': z}, device_id_type=MESH_ID)

    def kv_local(k):
        return pltpu.make_async_copy(kvst.at[k, stage], kv_out.at[stage, col, k], kv_self.at[k])

    def nb_copy():
        return pltpu.make_async_remote_copy(src_ref=kvst.at[0], dst_ref=nb, send_sem=nb_send, recv_sem=nb_recv,
                                            device_id={'model2': lax.rem(col + 1, width)}, device_id_type=MESH_ID)

    def row_copy(d, src_col):
        c, z = peer(d)
        return pltpu.make_async_remote_copy(src_ref=rowbuf, dst_ref=rland.at[src_col], send_sem=row_send.at[d], recv_sem=row_recv.at[src_col],
                                            device_id={'model': c, 'model2': z}, device_id_type=MESH_ID)

    def h_copy(d, src_col):
        return pltpu.make_async_remote_copy(src_ref=hsel, dst_ref=hg.at[src_col], send_sem=h_send.at[d], recv_sem=h_recv.at[src_col],
                                            device_id={'model2': lax.rem(col + d, width)}, device_id_type=MESH_ID)

    def p_copy(d, src_col):
        z = lax.rem(col + d, width)
        return pltpu.make_async_remote_copy(src_ref=yparts.at[z], dst_ref=yrecv.at[src_col], send_sem=p_send.at[d], recv_sem=p_recv.at[src_col],
                                            device_id={'model2': z}, device_id_type=MESH_ID)

    lane_r = lax.broadcasted_iota(jnp.int32, (rows, 128), 1)
    low = lane_r < 64

    def stack(c, base, packed):
        n = packed.shape[0]
        lo = low[:n]
        turned = pltpu.roll(packed, 64, 1)
        zero = jnp.zeros_like(packed)
        kst[c, base:base + n, :] = jnp.where(lo, packed, zero).astype(bf16)
        kst[c, KEYS + base:KEYS + base + n, :] = jnp.where(lo, zero, turned).astype(bf16)
        vst[c, base:base + n, :] = jnp.where(lo, turned, zero).astype(bf16)
        vst[c, KEYS + base:KEYS + base + n, :] = jnp.where(lo, zero, packed).astype(bf16)

    def keys_values(k, slot):
        kv = dot32(hbuf[...], wbuf[slot])
        half = kv.shape[1] // 2
        keys = rope_block(kv[:, :half], cosb[...], sinb[...])
        for c in range(stages):
            kt = keys[c // 2]
            vt = kv[:, half + (c // 2) * 128:half + (c // 2 + 1) * 128]
            if c % 2 == 0:
                packed = jnp.where(low, kt, pltpu.roll(vt, 64, 1))
            else:
                packed = jnp.where(low, pltpu.roll(kt, 64, 1), vt)
            packed = packed.astype(bf16)
            kvst[k, c] = packed
            stack(c, 0, packed.astype(f32))

        @pl.when(k == 0)
        def _():
            pl.semaphore_wait(barrier, n_dev - 1)

            @pl.when(lax.rem(col, 2) == 0)
            def _():
                nb_copy().start()

        kv_local(k).start()

        use_nb = (k == num_k - 1) & (lax.rem(col, 2) == 1)

        @pl.when(use_nb)
        def _():
            nb_copy().wait_recv()
            for c in range(stages):
                stack(c, KEYS // 2, nb[c, :chunk].astype(f32))

        @pl.when((k > 0) & jnp.logical_not(use_nb))
        def _():
            for c in range(stages):
                stack(c, KEYS // 2, kvst[lax.max(k - 1, 0), c, :chunk].astype(f32))

    def attend(q_ref, o_ref, m_ref, n_keys):
        per_c = q_cols // 128 // stages

        def group(c, carry):
            for i in range(per_c):
                at = pl.ds(pl.multiple_of((c * per_c + i) * 128, 128), 128)
                q = q_ref[:, at]
                out = None
                for e in range(2):
                    ks = slice(e * KEYS, e * KEYS + n_keys)
                    se = jnp.where(m_ref[:, :n_keys] > 0.5, dot32t(q, kst[c, ks]), NEG)
                    ex = jnp.exp(se - jnp.max(se, axis=-1, keepdims=True))
                    inv = 1.0 / jnp.sum(ex, axis=-1, keepdims=True)
                    part = dot32((ex * inv).astype(bf16), vst[c, ks])
                    out = part if out is None else out + part
                o_ref[:, at] = out.astype(bf16)
            return carry
        lax.fori_loop(0, stages, group, 0)

    def attend_chunk(k, q_ref, o_ref, m_ref):
        half = here(k, half_tab)

        @pl.when(half == 0)
        def _():
            attend(q_ref, o_ref, m_ref, KEYS // 2)

        @pl.when(half == 1)
        def _():
            attend(q_ref, o_ref, m_ref, KEYS)

    scale = 64 ** -0.5

    def block_at(j):
        return pl.ds(pl.multiple_of(j * BLK, BLK), BLK)

    def act_of(h, slot_g, slot_u):
        g = dot32(h, wbuf[slot_g])
        u = dot32(h, wbuf[slot_u])
        return (g * jax.nn.sigmoid(g) * u).astype(bf16)

    @pl.when(stage < last_stage)
    def _():
        total = per * num_k

        def one_chunk(k, carry):
            g0 = k * per
            set_tables(k)
            wait_x(k)
            hbuf[...] = norm_rows(xin[k].astype(f32), ga_ref[...])
            keys_values(k, landed(g0))
            refill(g0, total)

            def q_block(j, cc):
                g = g0 + 1 + j
                slot = landed(g)
                v = rope_block(dot32(hbuf[...], wbuf[slot]), cosb[...], sinb[...])
                for i in range(BLK // 128):
                    qbuf[:, pl.ds(pl.multiple_of(j * BLK + i * 128, 128), 128)] = (v[i] * scale).astype(bf16)
                refill(g, total)
                return cc
            lax.fori_loop(0, n_q, q_block, 0)

            attend_chunk(k, qbuf, obuf, maskb)

            def o_block(j, cc):
                g = g0 + 1 + n_q + j
                slot = landed(g)
                kv_copy(k, 1 + j, me).start()
                x1buf[:, block_at(j)] = (xin[k, :, block_at(j)].astype(f32) + dot32(obuf[...], wbuf[slot])).astype(bf16)
                refill(g, total)
                return cc
            lax.fori_loop(0, n_o, o_block, 0)

            x1 = x1buf[...].astype(f32)
            hbuf[...] = norm_rows(x1, gm_ref[...])
            yacc[...] = jnp.zeros_like(yacc)

            gf = g0 + 1 + n_q + n_o

            def up(j, slot):
                abuf[slot] = act_of(hbuf[...], wslot(gf + 3 * j), wslot(gf + 3 * j + 1))

            def down(j, slot):
                yacc[...] += dot32t(abuf[slot], wbuf[wslot(gf + 3 * j + 2)])

            landed(gf)
            landed(gf + 1)
            up(0, 0)
            refill(gf, total)
            refill(gf + 1, total)

            def f_pair(t, cc):
                j = 2 * t + 1
                for b in range(6):
                    landed(gf + 3 * j - 1 + b)
                kv_copy(k, n_o + j, me).start()
                kv_copy(k, n_o + j + 1, me).start()
                up(j, 1)
                down(j - 1, 0)
                up(j + 1, 0)
                down(j, 1)
                for b in range(6):
                    refill(gf + 3 * j - 1 + b, total)
                return cc
            lax.fori_loop(0, n_f // 2, f_pair, 0)
            kv_copy(k, n_dev - 1, me).start()
            landed(gf + 3 * n_f - 1)
            down(n_f - 1, 0)
            refill(gf + 3 * n_f - 1, total)
            ysend[k] = (x1buf[...].astype(f32) + yacc[...]).astype(bf16)
            act_copy(k).start()
            return carry
        lax.fori_loop(0, num_k, one_chunk, 0)

    @pl.when(stage == last_stage)
    def _():
        x6[...] = jnp.zeros_like(x6)
        o6[...] = jnp.zeros_like(o6)
        row_id = iota((small, q_cols), 0)
        for b in range(n_q + 1):
            landed(b)

        def one_chunk(k, carry):
            set_tables(k)
            wait_x(k)
            hbuf[...] = norm_rows(xin[k].astype(f32), ga_ref[...])
            keys_values(k, 0)

            def send(d, cc):
                kv_copy(k, d, me).start()
                return cc
            lax.fori_loop(1, n_dev, send, 0)
            r = iota((small, rows), 0)
            last_i = lax.clamp(0, here(k, len_tab) - 1 - here(k, half_tab) * chunk, chunk - 1)
            pick = jnp.where(r % 2 == 1, chunk, last_i)
            sel = jnp.where((r // 2 == k) & (iota((small, rows), 1) == pick), 1.0, 0.0).astype(bf16)
            x6[...] += dot32(sel, xin[k])
            hs = dot32(sel, hbuf[...]).astype(bf16)

            def q_block(j, cc):
                v = rope_block(dot32(hs, wbuf[1 + j]), coslb[...], sinlb[...])
                for i in range(BLK // 128):
                    qbuf[:small, pl.ds(pl.multiple_of(j * BLK + i * 128, 128), 128)] = (v[i] * scale).astype(bf16)
                return cc
            lax.fori_loop(0, n_q, q_block, 0)
            attend(qbuf.at[:small], obuf.at[:small], masklb, KEYS)
            o6[...] = jnp.where(row_id // 2 == k, obuf[:small].astype(f32), o6[...])
            return carry
        lax.fori_loop(0, num_k, one_chunk, 0)
        for b in range(n_q + 1, n_last):
            landed(b)
        o_in = o6[...].astype(bf16)

        def o_block(j, cc):
            x1buf[:small, block_at(j)] = (x6[:, block_at(j)] + dot32(o_in, wbuf[1 + n_q + j])).astype(bf16)
            return cc
        lax.fori_loop(0, n_o, o_block, 0)
        x1 = x1buf[:small].astype(f32)
        hsel[...] = norm_rows(x1, gm_ref[...])
        for d in range(1, width):
            h_copy(d, col).start()
        hg[col] = hsel[...]
        for d in range(1, width):
            h_copy(d, lax.rem(col + d, width)).wait_recv()
        h_all = jnp.concatenate([hg[z].astype(f32) for z in range(width)], axis=0).astype(bf16)
        yacc[:width * small] = jnp.zeros((width * small, model_dim), f32)

        def f_block(i, cc):
            b = 1 + n_q + n_o + 3 * i

            @pl.when(col + width * i < n_f)
            def _():
                yacc[:width * small] += dot32t(act_of(h_all, b, b + 1), wbuf[b + 2])
            return cc
        lax.fori_loop(0, n_mine, f_block, 0)
        for z in range(width):
            yparts[z] = yacc[z * small:(z + 1) * small]
        for d in range(1, width):
            p_copy(d, col).start()
        yrecv[col] = yparts[col]
        for d in range(1, width):
            p_copy(d, lax.rem(col + d, width)).wait_recv()
        rowbuf[...] = (x1 + (yrecv[0] + yrecv[1] + yrecv[2] + yrecv[3])).astype(bf16)

        def send(d, carry):
            row_copy(d, col).start()
            return carry
        lax.fori_loop(1, n_dev, send, 0)
        rland[col] = rowbuf[...]

    def drain(d, carry):
        src = lax.rem(me + d, n_dev)
        for k in range(num_k):
            kv_copy(k, d, me).wait_send()
            kv_copy(k, d, src).wait_recv()
        return carry
    lax.fori_loop(1, n_dev, drain, 0)
    for k in range(num_k):
        kv_local(k).wait()

    @pl.when(lax.rem(col, 2) == 0)
    def _():
        nb_copy().wait_send()

    @pl.when(stage < last_stage)
    def _():
        for k in range(num_k):
            act_copy(k).wait_send()

    @pl.when(stage == last_stage)
    def _():
        for d in range(1, width):
            h_copy(d, col).wait_send()
            p_copy(d, col).wait_send()

        def sent(d, carry):
            row_copy(d, col).wait_send()
            return carry
        lax.fori_loop(1, n_dev, sent, 0)

    for z in range(width):
        @pl.when((stage < last_stage) | (col != z))
        def _():
            row_copy(1, z).wait_recv()

    first, second = {}, {}
    for k in range(num_k):
        for z in range(width):
            (second if CHUNKS[k][z][1] else first)[CHUNKS[k][z][0]] = (z, k)
    got = [rland[z].astype(f32) for z in range(width)]

    def row_of(place, odd):
        return got[place[0]][2 * place[1] + odd:2 * place[1] + odd + 1]
    batch = dec_out.shape[0]
    dec_out[...] = jnp.concatenate([row_of(second[p], 1) for p in range(batch)], axis=0).astype(bf16)
    last_out[...] = jnp.concatenate([jnp.where(lens[p // row_count, p % row_count] > chunk, row_of(second[p], 0), row_of(first[p], 0))
                                     for p in range(batch)], axis=0).astype(bf16)


def solution(mesh):
    stages = mesh.shape['model']
    width = mesh.shape['model2']
    stage_spec = P('model', None, None)
    in_specs = (P('replica', None, None, None), P('replica', None), P('replica', None),
                stage_spec, stage_spec, stage_spec, stage_spec, P(None, None), P(None, None),
                P(None, None, TP_AXES, None), P(None, None, TP_AXES, None), P(None, None, TP_AXES, None),
                P(None, TP_AXES, None, None), P(None, None, TP_AXES), P(None, None, TP_AXES), P(None, TP_AXES, None))
    cache_spec = P(None, 'replica', None, TP_AXES, None)
    out_specs = (P('replica', None), P('replica', None), cache_spec, cache_spec)
    num_k = len(CHUNKS)
    def shard_body(x_prompt, lengths, x_new, st_qkv, st_out, st_gateup, st_down_t, gain_attn, gain_mlp, tp_query, tp_key, tp_value, tp_out, tp_gate, tp_up, tp_down):
        seq_len, model_dim = x_prompt.shape[2:]
        batch = x_new.shape[0]
        head_dim = tp_query.shape[-1]
        w_qkv, w_out, w_gateup, w_down_t = st_qkv[0], st_out[0], st_gateup[0], st_down_t[0]
        q_cols = w_out.shape[0]
        ff = w_down_t.shape[1]
        chunk = seq_len // 2
        rows = chunk + 16
        small = 8
        half_dim = head_dim // 2
        inv_freq = np.power(np.float32(THETA), np.arange(half_dim, dtype=np.float32) * np.float32(-2.0 / head_dim)).astype(np.float32)
        angles = (np.arange(seq_len + 8, dtype=np.float32)[:, None] * inv_freq).astype(np.float32)
        cos_h, sin_h = np.cos(angles).astype(np.float32), np.sin(angles).astype(np.float32)
        tab_cos = jnp.asarray(np.concatenate([cos_h] * 4, axis=1))
        tab_sin = jnp.asarray(np.concatenate([-sin_h, sin_h] * 2, axis=1))

        dims = (stages, width, num_k, rows, chunk, model_dim, q_cols, ff)
        bf16, f32 = jnp.bfloat16, jnp.float32
        n_dev = stages * width
        vm = pl.BlockSpec(memory_space=pltpu.VMEM)
        hbm = pl.BlockSpec(memory_space=pl.ANY)
        dma = pltpu.SemaphoreType.DMA
        kv_all, dec, last = pl.pallas_call(
            functools.partial(mega_kernel, dims),
            out_shape=(jax.ShapeDtypeStruct((stages, width, num_k, rows, 128), bf16),
                       jax.ShapeDtypeStruct((batch, model_dim), bf16), jax.ShapeDtypeStruct((batch, model_dim), bf16)),
            in_specs=[pl.BlockSpec(memory_space=pltpu.SMEM), hbm] + [vm] * 5 + [hbm] * 4,
            out_specs=(hbm, vm, vm),
            scratch_shapes=[
                pltpu.VMEM((NBUF, model_dim, BLK), bf16),
                pltpu.VMEM((num_k, rows, model_dim), bf16),
                pltpu.VMEM((num_k, rows, model_dim), bf16),
                pltpu.VMEM((num_k, stages, rows, 128), bf16),
                pltpu.VMEM((stages, rows, 128), bf16),
                pltpu.VMEM((stages, 2 * KEYS, 128), bf16),
                pltpu.VMEM((stages, 2 * KEYS, 128), bf16),
                pltpu.VMEM((rows, q_cols), bf16),
                pltpu.VMEM((rows, q_cols), bf16),
                pltpu.VMEM((rows, model_dim), bf16),
                pltpu.VMEM((rows, model_dim), bf16),
                pltpu.VMEM((rows, model_dim), f32),
                pltpu.VMEM((2, rows, BLK), bf16),
                pltpu.VMEM((rows, 128), f32),
                pltpu.VMEM((rows, 128), f32),
                pltpu.VMEM((rows, KEYS), f32),
                pltpu.VMEM((small, 128), f32),
                pltpu.VMEM((small, 128), f32),
                pltpu.VMEM((small, KEYS), f32),
                pltpu.VMEM((small, model_dim), bf16),
                pltpu.VMEM((small, model_dim), f32),
                pltpu.VMEM((small, q_cols), f32),
                pltpu.VMEM((width, small, model_dim), bf16),
                pltpu.VMEM((width, small, model_dim), f32),
                pltpu.VMEM((width, small, model_dim), f32),
                pltpu.VMEM((small, model_dim), bf16),
                pltpu.VMEM((width, small, model_dim), bf16),
                dma((NBUF,)), dma((num_k,)), dma((num_k,)), dma((num_k * n_dev,)), dma((num_k * n_dev,)), dma((num_k,)),
                dma, dma, dma((n_dev,)), dma((width,)), dma((width,)), dma((width,)), dma((width,)), dma((width,)),
            ],
            compiler_params=pltpu.CompilerParams(collective_id=0, has_side_effects=True, vmem_limit_bytes=67043328),
            name='pipeline',
        )(lengths, x_prompt, x_new, tab_cos, tab_sin, gain_attn, gain_mlp, w_qkv, w_out, w_gateup, w_down_t)

        where_a = {}
        where_b = {}
        for k in range(num_k):
            for z in range(width):
                (where_b if CHUNKS[k][z][1] else where_a)[CHUNKS[k][z][0]] = (z, k)
        full_kv = jnp.stack([jnp.concatenate([kv_all[:, where_a[p][0], where_a[p][1], :chunk],
                                              kv_all[:, where_b[p][0], where_b[p][1], :chunk + 1]], axis=1)
                             for p in range(batch)], axis=1)
        k_full = full_kv[:, :, :, None, :head_dim]
        v_full = full_kv[:, :, :, None, head_dim:]
        return dec, last, k_full, v_full

    return jax.shard_map(shard_body, mesh=mesh, in_specs=in_specs, out_specs=out_specs, check_vma=False)
```

```python
import functools

import jax
import jax.numpy as jnp
import numpy as np
from jax import lax
from jax.experimental import pallas as pl
from jax.experimental.pallas import tpu as pltpu
from jax.sharding import PartitionSpec as P

EPS = 1e-5
THETA = 10000.0
TP_AXES = ('model', 'model2')
NEG = -1e30
BLK = 512
NBUF = 18
KEYS = 512
MESH_ID = pl.DeviceIdType.MESH

CHUNKS = (((4, 0), (1, 0), (5, 0), (3, 0)),
          ((0, 0), (1, 1), (2, 0), (3, 1)),
          ((0, 1), (4, 1), (2, 1), (5, 1)))


def dot32(a, b):
    return jnp.dot(a, b, preferred_element_type=jnp.float32)


def dot32t(a, b):
    return lax.dot_general(a, b, (((1,), (1,)), ((), ())), preferred_element_type=jnp.float32)


def norm_rows(x_f32, gain):
    inv_rms = lax.rsqrt(jnp.mean(x_f32 * x_f32, axis=-1, keepdims=True) + EPS)
    return (x_f32 * inv_rms * gain).astype(jnp.bfloat16)


def rope_block(v, cos_t, sin_t):
    lane = lax.broadcasted_iota(jnp.int32, (v.shape[0], 128), 1)
    first = (lane % 64) < 32
    out = []
    for c in range(v.shape[1] // 128):
        t = v[:, c * 128:(c + 1) * 128]
        other = jnp.where(first, pltpu.roll(t, 96, 1), pltpu.roll(t, 32, 1))
        out.append(t * cos_t + other * sin_t)
    return out


def mega_kernel(dims, lens, x_prompt, x_new, tab_cos, tab_sin, ga_all, gm_all,
                w_qkv, w_out, w_gu, w_dt, kv_out, dec_out, last_out,
                wbuf, xin, ysend, kvst, nb, kst, vst, qbuf, obuf, hbuf, x1buf, yacc, abuf, cosb, sinb, maskb, coslb, sinlb, masklb,
                hsel, x6, o6, hg, yparts, yrecv, rowbuf, rland,
                wsem, act_send, act_recv, kv_send, kv_recv, kv_self, nb_send, nb_recv, row_send, row_recv,
                h_send, h_recv, p_send, p_recv):
    stages, width, num_k, rows, chunk, model_dim, q_cols, ff = dims
    n_dev = stages * width
    n_q = q_cols // BLK
    n_o = model_dim // BLK
    n_f = ff // BLK
    per = n_q + 1 + n_o + 3 * n_f
    stage = lax.axis_index('model')
    col = lax.axis_index('model2')
    me = stage * width + col
    last_stage = stages - 1
    f32 = jnp.float32
    bf16 = jnp.bfloat16
    small = x6.shape[0]
    row_count = x_prompt.shape[1]
    ga_ref = ga_all.at[pl.ds(stage, 1)]
    gm_ref = gm_all.at[pl.ds(stage, 1)]

    def here(k, table):
        out = table[0][0]
        for kk in range(num_k):
            for z in range(width):
                out = jnp.where((k == kk) & (col == z), table[kk][z], out)
        return out

    len_tab = [[lens[p // row_count, p % row_count] for p, _ in line] for line in CHUNKS]
    half_tab = [[h for _, h in line] for line in CHUNKS]

    def iota(shape, dim):
        return lax.broadcasted_iota(jnp.int32, shape, dim)

    def visible(j, pos, dec, length, half):
        ctx = KEYS // 2
        kpos = jnp.where(j < ctx, half * chunk + j, j - ctx)
        there = (j < chunk) | ((j >= ctx) & (j < ctx + half * chunk))
        seen = there & (kpos < length) & (dec | (kpos <= pos))
        return jnp.where(seen | (dec & (j == chunk)), 1.0, 0.0)

    def set_tables(k):
        length, half = here(k, len_tab), here(k, half_tab)
        at = pl.ds(pl.multiple_of(half * chunk, 8), chunk)
        t_i = iota(tab_cos.shape, 0)
        odd = iota((small, 128), 0) % 2 == 1
        for tab, buf, buf_l in ((tab_cos, cosb, coslb), (tab_sin, sinb, sinlb)):
            buf[:chunk] = tab[at, :]
            at_len = jnp.sum(jnp.where(t_i == length, tab[...], 0.0), axis=0, keepdims=True)
            buf[chunk:] = jnp.broadcast_to(at_len, (rows - chunk, 128))

            @pl.when(stage == last_stage)
            def _():
                at_last = jnp.sum(jnp.where(t_i == length - 1, tab[...], 0.0), axis=0, keepdims=True)
                buf_l[...] = jnp.where(odd, at_len, at_last)

        @pl.when(stage < last_stage)
        def _():
            i = iota((rows, KEYS), 0)
            dec = i >= chunk
            maskb[...] = visible(iota((rows, KEYS), 1), jnp.where(dec, length, half * chunk + i), dec, length, half)

        @pl.when(stage == last_stage)
        def _():
            dec = iota((small, KEYS), 0) % 2 == 1
            masklb[...] = visible(iota((small, KEYS), 1), jnp.where(dec, length, length - 1), dec, length, half)

    def wslot(g):
        return lax.rem(g, NBUF)

    def fetch(g):
        b = lax.rem(g, per)
        slot = wslot(g)

        def go(src, j):
            pltpu.make_async_copy(src.at[:, pl.ds(pl.multiple_of(j * BLK, BLK), BLK)], wbuf.at[slot], wsem.at[slot]).start()

        @pl.when(b == 0)
        def _():
            go(w_qkv, n_q)

        @pl.when((b >= 1) & (b <= n_q))
        def _():
            go(w_qkv, b - 1)

        @pl.when((b > n_q) & (b <= n_q + n_o))
        def _():
            go(w_out, b - n_q - 1)

        f = b - (n_q + n_o + 1)

        @pl.when((f >= 0) & (lax.rem(f, 3) == 0))
        def _():
            go(w_gu, f // 3)

        @pl.when((f >= 0) & (lax.rem(f, 3) == 1))
        def _():
            go(w_gu, n_f + f // 3)

        @pl.when((f >= 0) & (lax.rem(f, 3) == 2))
        def _():
            go(w_dt, f // 3)

    def fetch_last(b):
        def go(src, j):
            pltpu.make_async_copy(src.at[:, pl.ds(pl.multiple_of(j * BLK, BLK), BLK)], wbuf.at[b], wsem.at[b]).start()
        if b == 0:
            go(w_qkv, n_q)
        elif b <= n_q:
            go(w_qkv, b - 1)
        elif b <= n_q + n_o:
            go(w_out, b - n_q - 1)
        else:
            i = b - (n_q + n_o + 1)
            j = lax.min(col + (i // 3) * width, n_f - 1)
            if i % 3 == 0:
                go(w_gu, j)
            elif i % 3 == 1:
                go(w_gu, n_f + j)
            else:
                go(w_dt, j)

    def landed(g):
        slot = wslot(g)
        pltpu.make_async_copy(w_out.at[:, pl.ds(0, BLK)], wbuf.at[slot], wsem.at[slot]).wait()
        return slot

    def refill(g, total):
        @pl.when(g + NBUF < total)
        def _():
            fetch(g + NBUF)

    def first_fetch(g, carry):
        fetch(g)
        return carry
    n_mine = (n_f + width - 1) // width
    n_last = n_q + 1 + n_o + 3 * n_mine

    def x_copy(k, z):
        p, h = CHUNKS[k][z]
        return pltpu.make_async_copy(x_prompt.at[p // row_count, p % row_count, pl.ds(h * chunk, chunk)], xin.at[k, pl.ds(0, chunk)], act_recv.at[k])

    @pl.when(stage == 0)
    def _():
        for z in range(width):
            @pl.when(col == z)
            def _():
                for k in range(num_k):
                    x_copy(k, z).start()

    @pl.when(stage < last_stage)
    def _():
        lax.fori_loop(0, NBUF, first_fetch, 0)

    @pl.when(stage == last_stage)
    def _():
        for b in range(n_last):
            fetch_last(b)

    barrier = pltpu.get_barrier_semaphore()

    def peer(d):
        t = lax.rem(me + d, n_dev)
        return t // width, lax.rem(t, width)

    def greet(d, carry):
        c, z = peer(d)
        pl.semaphore_signal(barrier, inc=1, device_id={'model': c, 'model2': z}, device_id_type=MESH_ID)
        return carry
    lax.fori_loop(1, n_dev, greet, 0)

    @pl.when(stage == 0)
    def _():
        for z in range(width):
            @pl.when(col == z)
            def _():
                for k in range(num_k):
                    p = CHUNKS[k][z][0]
                    new_row = jnp.broadcast_to(x_new[p:p + 1, :].astype(f32), (rows - chunk, model_dim))
                    xin[k, chunk:] = jnp.where(iota(new_row.shape, 0) == 0, new_row, 0.0).astype(bf16)

    kst[...] = jnp.zeros_like(kst)
    vst[...] = jnp.zeros_like(vst)

    def wait_x(k):
        @pl.when(stage == 0)
        def _():
            pltpu.make_async_copy(x_prompt.at[0, 0, pl.ds(0, chunk)], xin.at[k, pl.ds(0, chunk)], act_recv.at[k]).wait()

        @pl.when(stage > 0)
        def _():
            act_copy(k).wait_recv()

    def act_copy(k):
        return pltpu.make_async_remote_copy(src_ref=ysend.at[k], dst_ref=xin.at[k], send_sem=act_send.at[k], recv_sem=act_recv.at[k],
                                            device_id={'model': lax.rem(stage + 1, stages)}, device_id_type=MESH_ID)

    def kv_copy(k, d, src_dev):
        c, z = peer(d)
        return pltpu.make_async_remote_copy(src_ref=kvst.at[k, c], dst_ref=kv_out.at[src_dev // width, lax.rem(src_dev, width), k],
                                            send_sem=kv_send.at[k * n_dev + d], recv_sem=kv_recv.at[src_dev * num_k + k],
                                            device_id={'model': c, 'model2': z}, device_id_type=MESH_ID)

    def kv_local(k):
        return pltpu.make_async_copy(kvst.at[k, stage], kv_out.at[stage, col, k], kv_self.at[k])

    def nb_copy():
        return pltpu.make_async_remote_copy(src_ref=kvst.at[0], dst_ref=nb, send_sem=nb_send, recv_sem=nb_recv,
                                            device_id={'model2': lax.rem(col + 1, width)}, device_id_type=MESH_ID)

    def row_copy(d, src_col):
        c, z = peer(d)
        return pltpu.make_async_remote_copy(src_ref=rowbuf, dst_ref=rland.at[src_col], send_sem=row_send.at[d], recv_sem=row_recv.at[src_col],
                                            device_id={'model': c, 'model2': z}, device_id_type=MESH_ID)

    def h_copy(d, src_col):
        return pltpu.make_async_remote_copy(src_ref=hsel, dst_ref=hg.at[src_col], send_sem=h_send.at[d], recv_sem=h_recv.at[src_col],
                                            device_id={'model2': lax.rem(col + d, width)}, device_id_type=MESH_ID)

    def p_copy(d, src_col):
        z = lax.rem(col + d, width)
        return pltpu.make_async_remote_copy(src_ref=yparts.at[z], dst_ref=yrecv.at[src_col], send_sem=p_send.at[d], recv_sem=p_recv.at[src_col],
                                            device_id={'model2': z}, device_id_type=MESH_ID)

    lane_r = lax.broadcasted_iota(jnp.int32, (rows, 128), 1)
    low = lane_r < 64

    def stack(c, base, packed):
        n = packed.shape[0]
        lo = low[:n]
        turned = pltpu.roll(packed, 64, 1)
        zero = jnp.zeros_like(packed)
        both = jnp.concatenate([packed, jnp.zeros((256 - n, 128), f32)], axis=0).T[:64]
        none = jnp.zeros_like(both)
        kst[c, :64, base:base + 256] = both.astype(bf16)
        kst[c, 64:, base:base + 256] = none.astype(bf16)
        kst[c, :64, KEYS + base:KEYS + base + 256] = none.astype(bf16)
        kst[c, 64:, KEYS + base:KEYS + base + 256] = both.astype(bf16)
        vst[c, base:base + n, :] = jnp.where(lo, turned, zero).astype(bf16)
        vst[c, KEYS + base:KEYS + base + n, :] = jnp.where(lo, zero, packed).astype(bf16)

    def keys_values(k, slot):
        kv = dot32(hbuf[...], wbuf[slot])
        half = kv.shape[1] // 2
        keys = rope_block(kv[:, :half], cosb[...], sinb[...])
        for c in range(stages):
            kt = keys[c // 2]
            vt = kv[:, half + (c // 2) * 128:half + (c // 2 + 1) * 128]
            if c % 2 == 0:
                packed = jnp.where(low, kt, pltpu.roll(vt, 64, 1))
            else:
                packed = jnp.where(low, pltpu.roll(kt, 64, 1), vt)
            packed = packed.astype(bf16)
            kvst[k, c] = packed
            stack(c, 0, packed.astype(f32))

        @pl.when(k == 0)
        def _():
            pl.semaphore_wait(barrier, n_dev - 1)

            @pl.when(lax.rem(col, 2) == 0)
            def _():
                nb_copy().start()

        kv_local(k).start()

        use_nb = (k == num_k - 1) & (lax.rem(col, 2) == 1)

        @pl.when(use_nb)
        def _():
            nb_copy().wait_recv()
            for c in range(stages):
                stack(c, KEYS // 2, nb[c, :chunk].astype(f32))

        @pl.when((k > 0) & jnp.logical_not(use_nb))
        def _():
            for c in range(stages):
                stack(c, KEYS // 2, kvst[lax.max(k - 1, 0), c, :chunk].astype(f32))

    per_c = q_cols // 128 // stages

    def attend(o_ref, m_ref, n_rows, n_keys):
        def group(c, carry):
            q = qbuf[c, :per_c * n_rows]
            seen = m_ref[:, :n_keys] > 0.5
            probs = []
            for e in range(2):
                s_all = dot32(q, kst[c, :, e * KEYS:e * KEYS + n_keys])
                for i in range(per_c):
                    se = jnp.where(seen, s_all[i * n_rows:(i + 1) * n_rows], NEG)
                    ex = jnp.exp(se - jnp.max(se, axis=-1, keepdims=True))
                    inv = 1.0 / jnp.sum(ex, axis=-1, keepdims=True)
                    probs.append((ex * inv).astype(bf16))
            out = dot32(jnp.concatenate(probs[:per_c], axis=0), vst[c, :n_keys]) + dot32(jnp.concatenate(probs[per_c:], axis=0), vst[c, KEYS:KEYS + n_keys])
            for i in range(per_c):
                o_ref[:, pl.ds(pl.multiple_of((c * per_c + i) * 128, 128), 128)] = out[i * n_rows:(i + 1) * n_rows].astype(bf16)
            return carry
        lax.fori_loop(0, stages, group, 0)

    def attend_chunk(k, o_ref, m_ref):
        half = here(k, half_tab)

        @pl.when(half == 0)
        def _():
            attend(o_ref, m_ref, rows, KEYS // 2)

        @pl.when(half == 1)
        def _():
            attend(o_ref, m_ref, rows, KEYS)

    scale = 64 ** -0.5

    def block_at(j):
        return pl.ds(pl.multiple_of(j * BLK, BLK), BLK)

    def act_of(h, slot_g, slot_u):
        g = dot32(h, wbuf[slot_g])
        u = dot32(h, wbuf[slot_u])
        return (g * jax.nn.sigmoid(g) * u).astype(bf16)

    @pl.when(stage < last_stage)
    def _():
        total = per * num_k

        def one_chunk(k, carry):
            g0 = k * per
            set_tables(k)
            wait_x(k)
            hbuf[...] = norm_rows(xin[k].astype(f32), ga_ref[...])
            keys_values(k, landed(g0))
            refill(g0, total)

            def q_block(j, cc):
                g = g0 + 1 + j
                slot = landed(g)
                v = rope_block(dot32(hbuf[...], wbuf[slot]), cosb[...], sinb[...])
                for i in range(BLK // 128):
                    qbuf[j, i * rows:(i + 1) * rows] = (v[i] * scale).astype(bf16)
                refill(g, total)
                return cc
            lax.fori_loop(0, n_q, q_block, 0)

            attend_chunk(k, obuf, maskb)

            def o_block(j, cc):
                g = g0 + 1 + n_q + j
                slot = landed(g)
                kv_copy(k, 1 + j, me).start()
                x1buf[:, block_at(j)] = (xin[k, :, block_at(j)].astype(f32) + dot32(obuf[...], wbuf[slot])).astype(bf16)
                refill(g, total)
                return cc
            lax.fori_loop(0, n_o, o_block, 0)

            x1 = x1buf[...].astype(f32)
            hbuf[...] = norm_rows(x1, gm_ref[...])
            yacc[...] = jnp.zeros_like(yacc)

            gf = g0 + 1 + n_q + n_o

            def up(j, slot):
                abuf[slot] = act_of(hbuf[...], wslot(gf + 3 * j), wslot(gf + 3 * j + 1))

            def down(j, slot):
                yacc[...] += dot32t(abuf[slot], wbuf[wslot(gf + 3 * j + 2)])

            landed(gf)
            landed(gf + 1)
            up(0, 0)
            refill(gf, total)
            refill(gf + 1, total)

            def f_pair(t, cc):
                j = 2 * t + 1
                for b in range(6):
                    landed(gf + 3 * j - 1 + b)
                kv_copy(k, n_o + j, me).start()
                kv_copy(k, n_o + j + 1, me).start()
                up(j, 1)
                down(j - 1, 0)
                up(j + 1, 0)
                down(j, 1)
                for b in range(6):
                    refill(gf + 3 * j - 1 + b, total)
                return cc
            lax.fori_loop(0, n_f // 2, f_pair, 0)
            kv_copy(k, n_dev - 1, me).start()
            landed(gf + 3 * n_f - 1)
            down(n_f - 1, 0)
            refill(gf + 3 * n_f - 1, total)
            ysend[k] = (x1buf[...].astype(f32) + yacc[...]).astype(bf16)
            act_copy(k).start()
            return carry
        lax.fori_loop(0, num_k, one_chunk, 0)

    @pl.when(stage == last_stage)
    def _():
        x6[...] = jnp.zeros_like(x6)
        o6[...] = jnp.zeros_like(o6)
        row_id = iota((small, q_cols), 0)
        for b in range(n_q + 1):
            landed(b)

        def one_chunk(k, carry):
            set_tables(k)
            wait_x(k)
            hbuf[...] = norm_rows(xin[k].astype(f32), ga_ref[...])
            keys_values(k, 0)

            def send(d, cc):
                kv_copy(k, d, me).start()
                return cc
            lax.fori_loop(1, n_dev, send, 0)
            r = iota((small, rows), 0)
            last_i = lax.clamp(0, here(k, len_tab) - 1 - here(k, half_tab) * chunk, chunk - 1)
            pick = jnp.where(r % 2 == 1, chunk, last_i)
            sel = jnp.where((r // 2 == k) & (iota((small, rows), 1) == pick), 1.0, 0.0).astype(bf16)
            x6[...] += dot32(sel, xin[k])
            hs = dot32(sel, hbuf[...]).astype(bf16)

            def q_block(j, cc):
                v = rope_block(dot32(hs, wbuf[1 + j]), coslb[...], sinlb[...])
                qbuf[j, :per_c * small] = (jnp.concatenate(v, axis=0) * scale).astype(bf16)
                return cc
            lax.fori_loop(0, n_q, q_block, 0)
            attend(obuf.at[:small], masklb, small, KEYS)
            o6[...] = jnp.where(row_id // 2 == k, obuf[:small].astype(f32), o6[...])
            return carry
        lax.fori_loop(0, num_k, one_chunk, 0)
        for b in range(n_q + 1, n_last):
            landed(b)
        o_in = o6[...].astype(bf16)

        def o_block(j, cc):
            x1buf[:small, block_at(j)] = (x6[:, block_at(j)] + dot32(o_in, wbuf[1 + n_q + j])).astype(bf16)
            return cc
        lax.fori_loop(0, n_o, o_block, 0)
        x1 = x1buf[:small].astype(f32)
        hsel[...] = norm_rows(x1, gm_ref[...])
        for d in range(1, width):
            h_copy(d, col).start()
        hg[col] = hsel[...]
        for d in range(1, width):
            h_copy(d, lax.rem(col + d, width)).wait_recv()
        h_all = jnp.concatenate([hg[z].astype(f32) for z in range(width)], axis=0).astype(bf16)
        yacc[:width * small] = jnp.zeros((width * small, model_dim), f32)

        def f_block(i, cc):
            b = 1 + n_q + n_o + 3 * i

            @pl.when(col + width * i < n_f)
            def _():
                yacc[:width * small] += dot32t(act_of(h_all, b, b + 1), wbuf[b + 2])
            return cc
        lax.fori_loop(0, n_mine, f_block, 0)
        for z in range(width):
            yparts[z] = yacc[z * small:(z + 1) * small]
        for d in range(1, width):
            p_copy(d, col).start()
        yrecv[col] = yparts[col]
        for d in range(1, width):
            p_copy(d, lax.rem(col + d, width)).wait_recv()
        rowbuf[...] = (x1 + (yrecv[0] + yrecv[1] + yrecv[2] + yrecv[3])).astype(bf16)

        def send(d, carry):
            row_copy(d, col).start()
            return carry
        lax.fori_loop(1, n_dev, send, 0)
        rland[col] = rowbuf[...]

    def drain(d, carry):
        src = lax.rem(me + d, n_dev)
        for k in range(num_k):
            kv_copy(k, d, me).wait_send()
            kv_copy(k, d, src).wait_recv()
        return carry
    lax.fori_loop(1, n_dev, drain, 0)
    for k in range(num_k):
        kv_local(k).wait()

    @pl.when(lax.rem(col, 2) == 0)
    def _():
        nb_copy().wait_send()

    @pl.when(stage < last_stage)
    def _():
        for k in range(num_k):
            act_copy(k).wait_send()

    @pl.when(stage == last_stage)
    def _():
        for d in range(1, width):
            h_copy(d, col).wait_send()
            p_copy(d, col).wait_send()

        def sent(d, carry):
            row_copy(d, col).wait_send()
            return carry
        lax.fori_loop(1, n_dev, sent, 0)

    for z in range(width):
        @pl.when((stage < last_stage) | (col != z))
        def _():
            row_copy(1, z).wait_recv()

    first, second = {}, {}
    for k in range(num_k):
        for z in range(width):
            (second if CHUNKS[k][z][1] else first)[CHUNKS[k][z][0]] = (z, k)
    got = [rland[z].astype(f32) for z in range(width)]

    def row_of(place, odd):
        return got[place[0]][2 * place[1] + odd:2 * place[1] + odd + 1]
    batch = dec_out.shape[0]
    dec_out[...] = jnp.concatenate([row_of(second[p], 1) for p in range(batch)], axis=0).astype(bf16)
    last_out[...] = jnp.concatenate([jnp.where(lens[p // row_count, p % row_count] > chunk, row_of(second[p], 0), row_of(first[p], 0))
                                     for p in range(batch)], axis=0).astype(bf16)


def solution(mesh):
    stages = mesh.shape['model']
    width = mesh.shape['model2']
    stage_spec = P('model', None, None)
    in_specs = (P('replica', None, None, None), P('replica', None), P('replica', None),
                stage_spec, stage_spec, stage_spec, stage_spec, P(None, None), P(None, None),
                P(None, None, TP_AXES, None), P(None, None, TP_AXES, None), P(None, None, TP_AXES, None),
                P(None, TP_AXES, None, None), P(None, None, TP_AXES), P(None, None, TP_AXES), P(None, TP_AXES, None))
    cache_spec = P(None, 'replica', None, TP_AXES, None)
    out_specs = (P('replica', None), P('replica', None), cache_spec, cache_spec)
    num_k = len(CHUNKS)
    def shard_body(x_prompt, lengths, x_new, st_qkv, st_out, st_gateup, st_down_t, gain_attn, gain_mlp, tp_query, tp_key, tp_value, tp_out, tp_gate, tp_up, tp_down):
        seq_len, model_dim = x_prompt.shape[2:]
        batch = x_new.shape[0]
        head_dim = tp_query.shape[-1]
        w_qkv, w_out, w_gateup, w_down_t = st_qkv[0], st_out[0], st_gateup[0], st_down_t[0]
        q_cols = w_out.shape[0]
        ff = w_down_t.shape[1]
        chunk = seq_len // 2
        rows = chunk + 16
        small = 8
        half_dim = head_dim // 2
        inv_freq = np.power(np.float32(THETA), np.arange(half_dim, dtype=np.float32) * np.float32(-2.0 / head_dim)).astype(np.float32)
        angles = (np.arange(seq_len + 8, dtype=np.float32)[:, None] * inv_freq).astype(np.float32)
        cos_h, sin_h = np.cos(angles).astype(np.float32), np.sin(angles).astype(np.float32)
        tab_cos = jnp.asarray(np.concatenate([cos_h] * 4, axis=1))
        tab_sin = jnp.asarray(np.concatenate([-sin_h, sin_h] * 2, axis=1))

        dims = (stages, width, num_k, rows, chunk, model_dim, q_cols, ff)
        bf16, f32 = jnp.bfloat16, jnp.float32
        n_dev = stages * width
        vm = pl.BlockSpec(memory_space=pltpu.VMEM)
        hbm = pl.BlockSpec(memory_space=pl.ANY)
        dma = pltpu.SemaphoreType.DMA
        kv_all, dec, last = pl.pallas_call(
            functools.partial(mega_kernel, dims),
            out_shape=(jax.ShapeDtypeStruct((stages, width, num_k, rows, 128), bf16),
                       jax.ShapeDtypeStruct((batch, model_dim), bf16), jax.ShapeDtypeStruct((batch, model_dim), bf16)),
            in_specs=[pl.BlockSpec(memory_space=pltpu.SMEM), hbm] + [vm] * 5 + [hbm] * 4,
            out_specs=(hbm, vm, vm),
            scratch_shapes=[
                pltpu.VMEM((NBUF, model_dim, BLK), bf16),
                pltpu.VMEM((num_k, rows, model_dim), bf16),
                pltpu.VMEM((num_k, rows, model_dim), bf16),
                pltpu.VMEM((num_k, stages, rows, 128), bf16),
                pltpu.VMEM((stages, rows, 128), bf16),
                pltpu.VMEM((stages, 128, 2 * KEYS), bf16),
                pltpu.VMEM((stages, 2 * KEYS, 128), bf16),
                pltpu.VMEM((stages, q_cols // 128 // stages * rows, 128), bf16),
                pltpu.VMEM((rows, q_cols), bf16),
                pltpu.VMEM((rows, model_dim), bf16),
                pltpu.VMEM((rows, model_dim), bf16),
                pltpu.VMEM((rows, model_dim), f32),
                pltpu.VMEM((2, rows, BLK), bf16),
                pltpu.VMEM((rows, 128), f32),
                pltpu.VMEM((rows, 128), f32),
                pltpu.VMEM((rows, KEYS), f32),
                pltpu.VMEM((small, 128), f32),
                pltpu.VMEM((small, 128), f32),
                pltpu.VMEM((small, KEYS), f32),
                pltpu.VMEM((small, model_dim), bf16),
                pltpu.VMEM((small, model_dim), f32),
                pltpu.VMEM((small, q_cols), f32),
                pltpu.VMEM((width, small, model_dim), bf16),
                pltpu.VMEM((width, small, model_dim), f32),
                pltpu.VMEM((width, small, model_dim), f32),
                pltpu.VMEM((small, model_dim), bf16),
                pltpu.VMEM((width, small, model_dim), bf16),
                dma((NBUF,)), dma((num_k,)), dma((num_k,)), dma((num_k * n_dev,)), dma((num_k * n_dev,)), dma((num_k,)),
                dma, dma, dma((n_dev,)), dma((width,)), dma((width,)), dma((width,)), dma((width,)), dma((width,)),
            ],
            compiler_params=pltpu.CompilerParams(collective_id=0, has_side_effects=True, vmem_limit_bytes=67043328),
            name='pipeline',
        )(lengths, x_prompt, x_new, tab_cos, tab_sin, gain_attn, gain_mlp, w_qkv, w_out, w_gateup, w_down_t)

        where_a = {}
        where_b = {}
        for k in range(num_k):
            for z in range(width):
                (where_b if CHUNKS[k][z][1] else where_a)[CHUNKS[k][z][0]] = (z, k)
        full_kv = jnp.stack([jnp.concatenate([kv_all[:, where_a[p][0], where_a[p][1], :chunk],
                                              kv_all[:, where_b[p][0], where_b[p][1], :chunk + 1]], axis=1)
                             for p in range(batch)], axis=1)
        k_full = full_kv[:, :, :, None, :head_dim]
        v_full = full_kv[:, :, :, None, head_dim:]
        return dec, last, k_full, v_full

    return jax.shard_map(shard_body, mesh=mesh, in_specs=in_specs, out_specs=out_specs, check_vma=False)
```
